256 devices in a mesh: seq: 32 (over z, x), chan: 8 (over y, core).
Axes of the slice: x: 4, y: 4, z: 8, core: 2. Of those that a mesh axis runs over, the one named last changes fastest.
Arguments:
- hidden: bfloat16 [8, 8192], replicated, may hold values from -6 to 6
- norm_gain: float32 [3, 8192], replicated, may hold values from 0.25 to 1.75
- in_weight: bfloat16 [2, 8192, 2, 16384], P(None, None, None, ('seq', 'chan')), may hold values from -0.25 to 0.25
- conv_weight: float32 [2, 4, 16384], P(None, None, ('seq', 'chan')), may hold values from -3 to 3
- conv_bias: float32 [2, 16384], P(None, ('seq', 'chan')), may hold values from -3 to 3
- conv_state: bfloat16 [2, 8, 3, 16384], P(None, None, None, ('seq', 'chan')), may hold values from -6 to 6
- xproj_weight: bfloat16 [2, 16384, 544], P(None, ('seq', 'chan')), may hold values from -0.09375 to 0.09375
- dt_weight: bfloat16 [2, 512, 16384], P(None, None, ('seq', 'chan')), may hold values from -0.25 to 0.25
- dt_bias: float32 [2, 16384], P(None, ('seq', 'chan')), may hold values from -4.6 to -2.3
- a_log: float32 [2, 16, 16384], P(None, None, ('seq', 'chan')), may hold values from 0 to 2.77
- skip_gain: float32 [2, 16384], P(None, ('seq', 'chan')), may hold values from 0.5 to 1.5
- ssm_state: float32 [2, 8, 16, 16384], P(None, None, None, ('seq', 'chan')), may hold values from -6 to 6
- out_weight: bfloat16 [2, 16384, 8192], P(None, ('seq', 'chan')), may hold values from -0.1875 to 0.1875
- asker_lookup_matrix: bfloat16 [8192, 8, 1280], P('seq', 'chan'), may hold values from -0.0625 to 0.0625
- o_weight: bfloat16 [8, 1024, 8192], P('chan', None, 'seq'), may hold values from -0.09375 to 0.09375
- kv_cache: bfloat16 [256, 256, 2, 8, 128], P('seq', None, None, 'chan'), may hold values from -64 to 64
- lengths: int32 [8], replicated, may hold values from 1 to 8192, as said below
- page_table: int32 [8, 32], replicated, may hold values from -1 to 255, as said below
Outputs:
- hidden_out: bfloat16 [8, 8192], P(None, ('seq', 'chan'))
- new_ssm: float32 [2, 8, 16, 16384], P(None, None, None, ('seq', 'chan'))
- new_conv: bfloat16 [2, 8, 3, 16384], P(None, None, None, ('seq', 'chan'))
- newest_pair: bfloat16 [8, 8, 2, 128], P(None, 'chan')
The draws below stay inside these ranges and needn't reach their ends.
Inputs may be any that keep to these rules, and one draw needn't show every extreme that they name: `lengths`: each request's context holds 1 to 8192 tokens; one request holds exactly 8192. page_table[b, j] for j < ceil(lengths[b] / 256) is the cache slot (index along seq times 8 plus the local slot) holding block j of request b; these slots are all different; every other entry is -1. Used slots are spread very unevenly: some devices along seq have all 8 of theirs used, others few or none.
All inputs are finite; a program needn't handle non-finite values.
Results may differ from the reference program's by a relative error of at most 0.018.
Values may be sent and summed in bfloat16 or wider, within the bound.
No kernel may reach another device: no remote copies, remote signals or barrier semaphores. Data moves between devices by JAX's collectives and lax.ppermute only.
A program may use at most 64 MiB of HBM per device.

```python
import jax
import jax.numpy as jnp
from jax import lax

D = 8192
E = 16384
N = 16
R = 512
KCONV = 4
HEADS = 64
KVH = 8
HD = 128
GROUP = 8
MAMBA_LAYERS = 2
REQ = 8
BLK = 256
PAGES_DEV = 8
SLOTS = 256
MAXPG = 32


def plan_pages(key):
    base_key = jax.random.fold_in(key, 11)
    pick_key, grow_key, ending_lock, jitter_key, rank_key = jax.random.split(base_key, 5)
    request_ids = jnp.arange(REQ, dtype=jnp.int32)
    longest = jax.random.randint(pick_key, (), 0, REQ, dtype=jnp.int32)
    short_most = (SLOTS // 2 - MAXPG) // REQ
    short_draw = jax.random.randint(grow_key, (REQ,), 0, short_most, dtype=jnp.int32)
    page_count = 1 + short_draw * short_draw // short_most
    page_count = jnp.where(request_ids == longest, MAXPG, page_count)
    tail_rows = jax.random.randint(ending_lock, (REQ,), 1, BLK + 1, dtype=jnp.int32)
    tail_rows = jnp.where(request_ids == longest, BLK, tail_rows)
    context = (page_count - 1) * BLK + tail_rows
    slot_ids = jnp.arange(SLOTS, dtype=jnp.int32)
    device_rank = jax.random.randint(rank_key, (SLOTS // PAGES_DEV,), 0, 8, dtype=jnp.int32)[slot_ids // PAGES_DEV]
    jitter = jax.random.randint(jitter_key, (SLOTS,), 0, 4096, dtype=jnp.int32)
    slot_score = (device_rank * 4096 + jitter) * SLOTS + slot_ids
    slot_order = jnp.argsort(slot_score).astype(jnp.int32)
    first_page = jnp.cumsum(page_count) - page_count
    column = jnp.arange(MAXPG, dtype=jnp.int32)
    flat_index = jnp.clip(first_page[:, None] + column[None, :], 0, SLOTS - 1)
    slot_table = jnp.where(column[None, :] < page_count[:, None], slot_order[flat_index], -1)
    return (context.astype(jnp.int32), slot_table.astype(jnp.int32))


def draw_lengths(key, part):
    return plan_pages(key)[0]


def draw_page_table(key, part):
    return plan_pages(key)[1]


def draw_kv_cache(key, part):
    cache_shape = (SLOTS, BLK, 2, KVH, HD)
    values = jnp.clip(jax.random.normal(key, cache_shape, jnp.float32), -6.0, 6.0)
    return values.astype(jnp.bfloat16)


def with_spikes(values, key, source, target, blocks, factor):
    owner, partner = [(jnp.arange(values.shape[dim]) // (values.shape[dim] // blocks)).reshape([-1 if axis == dim else 1 for axis in range(values.ndim)]) for dim in (source, target)]
    chosen = jax.random.permutation(key, blocks)[partner]
    strong = (owner == chosen) | (owner == (partner + blocks // 2) % blocks)
    return jnp.where(strong, factor * values, values)


def steps_of(key, dims, cuts, low, largest):
    level = 1.0
    for axis_at, parts in cuts:
        draws = jax.random.uniform(jax.random.fold_in(jax.random.fold_in(key, 6), axis_at), (parts,), jnp.float32, low / len(cuts), largest / len(cuts))
        level = level * jnp.repeat(jnp.exp(draws), dims[axis_at] // parts).reshape((-1,) + (1,) * (len(dims) - 1 - axis_at))
    return level


def bell_draw(rng, shape, deviation, limit, shards=(), kind=jnp.bfloat16):
    entries = deviation * jax.random.normal(rng, shape, jnp.float32)
    if shards:
        entries = entries * steps_of(rng, shape, shards, -0.22, 0.18)
    return jnp.clip(entries, -limit, limit).astype(kind)


def heavy_noise(key, shape, spread, most, cuts, heavy, kind=jnp.bfloat16):
    result = spread * jax.random.normal(key, shape, jnp.float32)
    if cuts:
        result = result * steps_of(key, shape, cuts, -0.22, 0.18)
    return jnp.clip(with_spikes(result, jax.random.fold_in(key, 3), *heavy), -most, most).astype(kind)


def setup_inputs(seed: int = 0) -> dict:
    key_of = jax.random.split(jax.random.key(seed), 19)
    hidden = bell_draw(key_of[0], (REQ, D), 1.0, 6.0)
    norm_gain = jnp.clip(1.0 + 0.15 * jax.random.normal(key_of[1], (3, D), jnp.float32), 0.25, 1.75)
    in_weight = heavy_noise(key_of[2], (MAMBA_LAYERS, D, 2, E), D ** -0.5, 0.25, ((3, 256),), (1, 3, 256, 6.0))
    conv_weight = bell_draw(key_of[3], (MAMBA_LAYERS, KCONV, E), KCONV ** -0.5, 3.0, ((2, 256),), jnp.float32)
    conv_bias = bell_draw(key_of[4], (MAMBA_LAYERS, E), 0.5, 3.0, ((1, 256),), jnp.float32)
    conv_state = bell_draw(key_of[5], (MAMBA_LAYERS, REQ, KCONV - 1, E), 1.0, 6.0, ((3, 256),))
    xproj_weight = heavy_noise(key_of[6], (MAMBA_LAYERS, E, R + 2 * N), E ** -0.5, 0.09375, ((1, 256),), (1, 2, 32, 2.75))
    dt_weight = bell_draw(key_of[7], (MAMBA_LAYERS, R, E), R ** -0.5, 0.25, ((2, 256),))
    dt_bias = jnp.clip(-4.6 + 2.3 * jax.random.uniform(key_of[8], (MAMBA_LAYERS, E), jnp.float32) ** steps_of(key_of[8], (MAMBA_LAYERS, E), ((1, 256),), -0.2, 0.2), -4.6, -2.3)
    a_log = jnp.clip(2.77 * jax.random.uniform(key_of[9], (MAMBA_LAYERS, N, E), jnp.float32) ** steps_of(key_of[9], (MAMBA_LAYERS, N, E), ((2, 256),), -0.2, 0.2), 0.0, 2.77)
    skip_gain = jnp.clip(0.5 + 1.0 * jax.random.uniform(key_of[10], (MAMBA_LAYERS, E), jnp.float32) ** steps_of(key_of[10], (MAMBA_LAYERS, E), ((1, 256),), -0.2, 0.2), 0.5, 1.5)
    ssm_state = bell_draw(key_of[11], (MAMBA_LAYERS, REQ, N, E), 1.0, 6.0, ((3, 256),), jnp.float32)
    out_weight = heavy_noise(key_of[12], (MAMBA_LAYERS, E, D), E ** -0.5, 0.1875, ((1, 256),), (1, 2, 256, 6.0))
    asker_lookup_matrix = bell_draw(key_of[13], (D, KVH, (GROUP + 2) * HD), D ** -0.5, 0.0625, ((0, 32), (1, 8)))
    o_weight = heavy_noise(key_of[14], (KVH, GROUP * HD, D), (HEADS * HD) ** -0.5, 0.09375, ((0, 8), (2, 32)), (0, 2, 8, 2.0))
    kv_cache = draw_kv_cache(jax.random.fold_in(key_of[18], 71), 0)
    lengths = draw_lengths(jax.random.fold_in(key_of[18], 71), 0)
    page_table = draw_page_table(jax.random.fold_in(key_of[18], 71), 0)
    return {"hidden": hidden, "norm_gain": norm_gain, "in_weight": in_weight, "conv_weight": conv_weight, "conv_bias": conv_bias, "conv_state": conv_state, "xproj_weight": xproj_weight, "dt_weight": dt_weight, "dt_bias": dt_bias, "a_log": a_log, "skip_gain": skip_gain, "ssm_state": ssm_state, "out_weight": out_weight, "asker_lookup_matrix": asker_lookup_matrix, "o_weight": o_weight, "kv_cache": kv_cache, "lengths": lengths, "page_table": page_table}


norm_eps = 1e-06
lowest_score = -1e+30

def normalize(stream, gain_row):
    widened = stream.astype(jnp.float32)
    inv_rms = lax.rsqrt(lax.optimization_barrier(jnp.mean(widened * widened, axis=1)) + norm_eps)
    return (widened * inv_rms[:, None] * gain_row[None, :]).astype(jnp.bfloat16)

def mamba_layer(stream, gain_row, layer, in_weight, conv_weight, conv_bias, conv_state, xproj_weight, dt_weight, dt_bias, a_log, skip_gain, ssm_state, out_weight):
    normed = normalize(stream, gain_row)
    channels = in_weight.shape[3]
    both_proj = jnp.dot(normed, in_weight[layer].reshape(in_weight.shape[1], 2 * channels), preferred_element_type=jnp.float32).astype(jnp.bfloat16)
    inputs = both_proj[:, :channels]
    gate_half = both_proj[:, channels:]
    window = jnp.concatenate([conv_state[layer], inputs[:, None, :]], axis=1)
    conv_sum = lax.optimization_barrier(jnp.sum(window.astype(jnp.float32) * conv_weight[layer][None], axis=1)) + conv_bias[layer][None, :]
    signal = lax.optimization_barrier(jax.nn.silu(conv_sum).astype(jnp.bfloat16))
    mapped_vectors = jnp.dot(signal, xproj_weight[layer], preferred_element_type=jnp.float32)
    low_rank = dt_weight.shape[1]
    state_size = a_log.shape[1]
    dt_low = mapped_vectors[:, :low_rank].astype(jnp.bfloat16)
    b_in = mapped_vectors[:, low_rank:low_rank + state_size]
    c_out = mapped_vectors[:, low_rank + state_size:]
    dt_step = jax.nn.softplus(jnp.dot(dt_low, dt_weight[layer], preferred_element_type=jnp.float32) + dt_bias[layer][None, :])
    widened = signal.astype(jnp.float32)
    decay_rate = jnp.exp(-dt_step[:, None, :] * jnp.exp(a_log[layer])[None])
    fresh_state = decay_rate * ssm_state[layer] + (dt_step * widened)[:, None, :] * b_in[:, :, None]
    readout = lax.optimization_barrier(jnp.sum(fresh_state * c_out[:, :, None], axis=1)) + skip_gain[layer][None, :] * widened
    gated_out = (readout * jax.nn.silu(gate_half.astype(jnp.float32))).astype(jnp.bfloat16)
    mixed_out = jnp.dot(gated_out, out_weight[layer], preferred_element_type=jnp.float32)
    return ((stream.astype(jnp.float32) + mixed_out).astype(jnp.bfloat16), fresh_state, window[:, 1:, :])

def attention_layer(stream, gain_row, asker_lookup_matrix, o_weight, kv_cache, lengths, page_table):
    normed = normalize(stream, gain_row)
    requests = stream.shape[0]
    heads_kv = asker_lookup_matrix.shape[1]
    per_lens_width = kv_cache.shape[4]
    group_size = asker_lookup_matrix.shape[2] // per_lens_width - 2
    inv_sqrt = per_lens_width ** (-0.5)
    qkv_all = jnp.dot(normed, asker_lookup_matrix.reshape(asker_lookup_matrix.shape[0], -1), preferred_element_type=jnp.float32)
    qkv_all = lax.optimization_barrier(qkv_all.astype(jnp.bfloat16)).reshape(requests, heads_kv, -1)
    every_question = qkv_all[:, :, :group_size * per_lens_width].reshape(requests, heads_kv, group_size, per_lens_width)
    newest_pair = qkv_all[:, :, group_size * per_lens_width:].reshape(requests, heads_kv, 2, per_lens_width)
    highest = lax.Precision.HIGHEST

    def attend_one(items):
        query_one, fresh_one, length_one, table_one = items
        page_rows = kv_cache[jnp.maximum(table_one, 0)]
        block_len = page_rows.shape[1]
        position = jnp.arange(table_one.shape[0], dtype=jnp.int32)[:, None] * block_len + jnp.arange(block_len, dtype=jnp.int32)[None, :]
        visible = (position < length_one)[None, None]
        scores = jnp.einsum('kgd,ptkd->kgpt', query_one.astype(jnp.float32), page_rows[:, :, 0].astype(jnp.float32), precision=highest) * inv_sqrt
        scores = jnp.where(visible, scores, lowest_score)
        block_top = lax.optimization_barrier(jnp.max(scores, axis=3))
        weight = jnp.where(visible, jnp.exp(scores - block_top[..., None]), 0.0)
        block_sum = lax.optimization_barrier(jnp.sum(weight, axis=3))
        rounded = lax.optimization_barrier(weight.astype(jnp.bfloat16)).astype(jnp.float32)
        block_val = jnp.einsum('kgpt,ptkd->kgpd', rounded, page_rows[:, :, 1].astype(jnp.float32), precision=highest)
        fresh_score = jnp.einsum('kgd,kd->kg', query_one.astype(jnp.float32), fresh_one[:, 0].astype(jnp.float32), precision=highest) * inv_sqrt
        final_top = jnp.maximum(lax.optimization_barrier(jnp.max(block_top, axis=2)), fresh_score)
        factor = jnp.exp(block_top - final_top[..., None])
        fresh_weight = jnp.exp(fresh_score - final_top)
        denominator = lax.optimization_barrier(jnp.sum(factor * block_sum, axis=2)) + fresh_weight
        numerator = jnp.einsum('kgp,kgpd->kgd', factor, block_val, precision=highest) + fresh_weight[..., None] * fresh_one[:, 1][:, None, :].astype(jnp.float32)
        return (numerator / denominator[..., None]).astype(jnp.bfloat16)
    attended = lax.map(attend_one, (every_question, newest_pair, lengths, page_table))
    mapped_vectors = jnp.dot(attended.reshape(requests, -1), o_weight.reshape(-1, o_weight.shape[2]), preferred_element_type=jnp.float32)
    return ((stream.astype(jnp.float32) + mapped_vectors).astype(jnp.bfloat16), newest_pair)

def reference(hidden, norm_gain, in_weight, conv_weight, conv_bias, conv_state, xproj_weight, dt_weight, dt_bias, a_log, skip_gain, ssm_state, out_weight, asker_lookup_matrix, o_weight, kv_cache, lengths, page_table):
    stream_one, state_first, conv_first = mamba_layer(hidden, norm_gain[0], 0, in_weight, conv_weight, conv_bias, conv_state, xproj_weight, dt_weight, dt_bias, a_log, skip_gain, ssm_state, out_weight)
    stream_two, newest_pair = attention_layer(stream_one, norm_gain[1], asker_lookup_matrix, o_weight, kv_cache, lengths, page_table)
    hidden_out, state_two, conv_two = mamba_layer(stream_two, norm_gain[2], 1, in_weight, conv_weight, conv_bias, conv_state, xproj_weight, dt_weight, dt_bias, a_log, skip_gain, ssm_state, out_weight)
    return (hidden_out, jnp.stack([state_first, state_two]), jnp.stack([conv_first, conv_two]), newest_pair)
```

```python
import jax
import jax.numpy as jnp
from jax import lax
from jax.sharding import Mesh
from jax.sharding import PartitionSpec as P

ALL = ("z", "x", "y", "core")
SEQ = ("z", "x")
CHAN = ("y", "core")
PLANE = ("x", "y")
LINE = ("z", "core")
WIRE = jnp.bfloat16

norm_eps = 1e-06
lowest_score = -1e30


def copy_for_each(x, axes):
    copies = jnp.broadcast_to(x, (lax.axis_size(axes), *x.shape))
    return lax.all_to_all(copies, axes, split_axis=0, concat_axis=0, tiled=True)


def of_everyone(x, axes):
    return jnp.sum(copy_for_each(x.astype(WIRE), axes).astype(jnp.float32), axis=0)


def normalize(stream, gain_row):
    widened = stream.astype(jnp.float32)
    inv_rms = lax.rsqrt(jnp.mean(widened * widened, axis=1) + norm_eps)
    return (widened * inv_rms[:, None] * gain_row[None, :]).astype(jnp.bfloat16)


def two_parts(x):
    high = x.astype(WIRE).astype(jnp.float32)
    return high, (x - high).astype(WIRE).astype(jnp.float32)


def mamba_mix(normed, layer, params):
    (
        in_weight,
        conv_weight,
        conv_bias,
        conv_state,
        xproj_weight,
        dt_weight,
        dt_bias,
        a_log,
        skip_gain,
        ssm_state,
    ) = params
    channels = in_weight.shape[3]
    both_proj = jnp.dot(
        normed,
        in_weight[layer].reshape(in_weight.shape[1], 2 * channels),
        preferred_element_type=jnp.float32,
    ).astype(jnp.bfloat16)
    inputs = both_proj[:, :channels]
    gate_half = both_proj[:, channels:]
    window = jnp.concatenate([conv_state[layer], inputs[:, None, :]], axis=1)
    conv_sum = (
        jnp.sum(window.astype(jnp.float32) * conv_weight[layer][None], axis=1)
        + conv_bias[layer][None, :]
    )
    signal = lax.optimization_barrier(jax.nn.silu(conv_sum).astype(jnp.bfloat16))
    x_terms = jnp.dot(signal, xproj_weight[layer], preferred_element_type=jnp.float32)
    mapped_vectors = of_everyone(of_everyone(x_terms, PLANE), LINE)
    low_rank = dt_weight.shape[1]
    state_size = a_log.shape[1]
    dt_low = mapped_vectors[:, :low_rank].astype(jnp.bfloat16)
    b_in = mapped_vectors[:, low_rank : low_rank + state_size]
    c_out = mapped_vectors[:, low_rank + state_size :]
    dt_step = jax.nn.softplus(
        jnp.dot(dt_low, dt_weight[layer], preferred_element_type=jnp.float32)
        + dt_bias[layer][None, :]
    )
    widened = signal.astype(jnp.float32)
    decay_rate = jnp.exp(-dt_step[:, None, :] * jnp.exp(a_log[layer])[None])
    fresh_state = decay_rate * ssm_state[layer] + (dt_step * widened)[:, None, :] * b_in[:, :, None]
    readout = jnp.sum(fresh_state * c_out[:, :, None], axis=1) + skip_gain[layer][None, :] * widened
    gated_out = (readout * jax.nn.silu(gate_half.astype(jnp.float32))).astype(jnp.bfloat16)
    return (gated_out, fresh_state, window[:, 1:, :])


def mix_out(gated_out, out_weight, layer):
    partial = jnp.dot(gated_out, out_weight[layer], preferred_element_type=jnp.float32)
    rows, dim = partial.shape
    parts = lax.axis_size(SEQ)
    blocks = partial.astype(WIRE).reshape(rows, parts, dim // parts).swapaxes(0, 1)
    arrived = lax.all_to_all(blocks, SEQ, split_axis=0, concat_axis=0, tiled=True)
    return of_everyone(jnp.sum(arrived.astype(jnp.float32), axis=0), CHAN)


def local_attention(questions, kv_cache, lengths, page_table, inv_sqrt):
    requests, group_size, width = questions.shape
    pages_dev, block_len = kv_cache.shape[:2]
    slot_ids = lax.axis_index(SEQ) * pages_dev + jnp.arange(pages_dev, dtype=jnp.int32)
    matches = page_table[:, :, None] == slot_ids[None, None, :]
    first_token = jnp.arange(page_table.shape[1], dtype=jnp.int32) * block_len
    left = jnp.clip(lengths[:, None] - first_token[None, :], 0, block_len)
    filled = jnp.sum(jnp.where(matches, left[:, :, None], 0), axis=1)
    visible = (
        jnp.arange(block_len, dtype=jnp.int32)[None, None, :] < filled[:, :, None]
    ).reshape(requests, 1, pages_dev * block_len)
    keys = kv_cache[:, :, 0, 0].reshape(pages_dev * block_len, width)
    values = kv_cache[:, :, 1, 0].reshape(pages_dev * block_len, width)
    scores = (
        jnp.dot(
            questions.reshape(requests * group_size, width),
            keys.T,
            preferred_element_type=jnp.float32,
        )
        * inv_sqrt
    ).reshape(requests, group_size, pages_dev * block_len)
    scores = jnp.where(visible, scores, lowest_score)
    high, low = two_parts(jnp.max(scores, axis=2))
    weight = jnp.where(visible, jnp.exp(scores - (high + low)[..., None]), 0.0)
    total = jnp.sum(weight, axis=2)
    mixed = jnp.dot(
        weight.astype(jnp.bfloat16).reshape(requests * group_size, pages_dev * block_len),
        values,
        preferred_element_type=jnp.float32,
    )
    return high, low, total, mixed


def attend(stream_one, gain_block, asker_lookup_matrix, kv_cache, lengths, page_table, model_dim):
    requests = stream_one.shape[0]
    width = kv_cache.shape[4]
    group_size = asker_lookup_matrix.shape[2] // width - 2
    entries = asker_lookup_matrix.shape[2]
    rows = requests * group_size
    inv_sqrt = width ** (-0.5)
    widened = stream_one.astype(jnp.float32)
    high, low = two_parts(jnp.sum(widened * widened, axis=1))
    scaled = (widened * gain_block[None, :]).astype(jnp.bfloat16)
    terms = jnp.dot(scaled, asker_lookup_matrix[:, 0, :], preferred_element_type=jnp.float32)
    summed = of_everyone(
        jnp.concatenate([terms, high[:, None], low[:, None], jnp.zeros((requests, 126))], axis=1),
        SEQ,
    )
    inv_rms = lax.rsqrt((summed[:, entries] + summed[:, entries + 1]) / model_dim + norm_eps)
    qkv = (summed[:, :entries] * inv_rms[:, None]).astype(jnp.bfloat16)
    questions = qkv[:, : group_size * width].reshape(requests, group_size, width)
    fresh_key = qkv[:, group_size * width : (group_size + 1) * width]
    fresh_value = qkv[:, (group_size + 1) * width :]
    newest_pair = jnp.stack([fresh_key, fresh_value], axis=1)[:, None]
    high, low, total, mixed = local_attention(questions, kv_cache, lengths, page_table, inv_sqrt)
    notes = jnp.stack([high.reshape(rows), low.reshape(rows), total.reshape(rows)])
    notes = jnp.pad(notes, ((0, 5), (0, width - rows)))
    packed = jnp.concatenate([mixed, notes], axis=0).astype(WIRE)
    arrived = copy_for_each(packed, SEQ).astype(jnp.float32)
    tops = (arrived[:, rows, :rows] + arrived[:, rows + 1, :rows]).reshape(
        -1, requests, group_size
    )
    totals = arrived[:, rows + 2, :rows].reshape(-1, requests, group_size)
    mixes = arrived[:, :rows].reshape(-1, requests, group_size, width)
    fresh_score = (
        jnp.sum(
            questions.astype(jnp.float32) * fresh_key[:, None, :].astype(jnp.float32), axis=2
        )
        * inv_sqrt
    )
    final_top = jnp.maximum(jnp.max(tops, axis=0), fresh_score)
    scale = jnp.exp(tops - final_top[None])
    fresh_weight = jnp.exp(fresh_score - final_top)
    denominator = jnp.sum(scale * totals, axis=0) + fresh_weight
    numerator = (
        jnp.sum(scale[..., None] * mixes, axis=0)
        + fresh_weight[..., None] * fresh_value[:, None, :].astype(jnp.float32)
    )
    attended = (numerator / denominator[..., None]).astype(jnp.bfloat16)
    return attended.reshape(requests, group_size * width), newest_pair


def shards(
    hidden,
    norm_gain,
    in_weight,
    conv_weight,
    conv_bias,
    conv_state,
    xproj_weight,
    dt_weight,
    dt_bias,
    a_log,
    skip_gain,
    ssm_state,
    out_weight,
    asker_lookup_matrix,
    o_weight,
    kv_cache,
    lengths,
    page_table,
):
    layer_params = (
        in_weight,
        conv_weight,
        conv_bias,
        conv_state,
        xproj_weight,
        dt_weight,
        dt_bias,
        a_log,
        skip_gain,
        ssm_state,
    )
    requests, model_dim = hidden.shape
    block_cols = model_dim // lax.axis_size(SEQ)
    share_cols = block_cols // lax.axis_size(CHAN)
    first_col = lax.axis_index(SEQ) * block_cols
    normed = normalize(hidden, norm_gain[0])
    gated_first, state_first, conv_first = mamba_mix(normed, 0, layer_params)
    own_block = lax.dynamic_slice_in_dim(hidden, first_col, block_cols, 1)
    gain_block = lax.dynamic_slice_in_dim(norm_gain[1], first_col, block_cols, 0)
    stream_one = (own_block.astype(jnp.float32) + mix_out(gated_first, out_weight, 0)).astype(
        jnp.bfloat16
    )
    attended, newest_pair = attend(
        stream_one, gain_block, asker_lookup_matrix, kv_cache, lengths, page_table, model_dim
    )
    attn_block = of_everyone(
        jnp.dot(attended, o_weight[0], preferred_element_type=jnp.float32), CHAN
    )
    stream_two = (stream_one.astype(jnp.float32) + attn_block).astype(jnp.bfloat16)
    whole_two = copy_for_each(stream_two, SEQ).swapaxes(0, 1).reshape(requests, model_dim)
    normed_two = normalize(whole_two, norm_gain[2])
    gated_two, state_two, conv_two = mamba_mix(normed_two, 1, layer_params)
    out_block = (stream_two.astype(jnp.float32) + mix_out(gated_two, out_weight, 1)).astype(
        jnp.bfloat16
    )
    hidden_out = lax.dynamic_slice_in_dim(
        out_block, lax.axis_index(CHAN) * share_cols, share_cols, 1
    )
    return (
        hidden_out,
        jnp.stack([state_first, state_two]),
        jnp.stack([conv_first, conv_two]),
        newest_pair,
    )


def solution(mesh):
    split = Mesh(mesh.devices.reshape(8, 4, 4, 2), ALL)
    placed = (
        P(),
        P(),
        P(None, None, None, ALL),
        P(None, None, ALL),
        P(None, ALL),
        P(None, None, None, ALL),
        P(None, ALL, None),
        P(None, None, ALL),
        P(None, ALL),
        P(None, None, ALL),
        P(None, ALL),
        P(None, None, None, ALL),
        P(None, ALL, None),
        P(SEQ, CHAN, None),
        P(CHAN, None, SEQ),
        P(SEQ, None, None, CHAN, None),
        P(),
        P(),
    )
    return jax.shard_map(
        shards,
        mesh=split,
        in_specs=placed,
        out_specs=(
            P(None, ALL),
            P(None, None, None, ALL),
            P(None, None, None, ALL),
            P(None, CHAN, None, None),
        ),
        check_vma=False,
    )
```

```python
import jax
import jax.numpy as jnp
from jax import lax
from jax.sharding import Mesh
from jax.sharding import PartitionSpec as P

ALL = ("z", "x", "y", "core")
SEQ = ("z", "x")
CHAN = ("y", "core")
PLANE = ("x", "y")
LINE = ("z", "core")
WIRE = jnp.bfloat16

norm_eps = 1e-06
lowest_score = -1e30


def copy_for_each(x, axes):
    copies = jnp.broadcast_to(x, (lax.axis_size(axes), *x.shape))
    return lax.all_to_all(copies, axes, split_axis=0, concat_axis=0, tiled=True)


def of_everyone(x, axes):
    return jnp.sum(copy_for_each(x.astype(WIRE), axes).astype(jnp.float32), axis=0)


def normalize(stream, gain_row):
    widened = stream.astype(jnp.float32)
    inv_rms = lax.rsqrt(jnp.mean(widened * widened, axis=1) + norm_eps)
    return (widened * inv_rms[:, None] * gain_row[None, :]).astype(jnp.bfloat16)


def two_parts(x):
    high = x.astype(WIRE).astype(jnp.float32)
    return high, (x - high).astype(WIRE).astype(jnp.float32)


def layer_values(layer, conv_weight, conv_bias, conv_state, dt_bias, a_log, skip_gain, ssm_state):
    return (
        conv_weight[layer],
        conv_bias[layer],
        conv_state[layer],
        dt_bias[layer],
        jnp.exp(a_log[layer]),
        skip_gain[layer],
        ssm_state[layer],
    )


def rows_in_use(pages_dev, block_len, lengths, page_table):
    slot_ids = lax.axis_index(SEQ) * pages_dev + jnp.arange(pages_dev, dtype=jnp.int32)
    matches = page_table[:, :, None] == slot_ids[None, None, :]
    first_token = jnp.arange(page_table.shape[1], dtype=jnp.int32) * block_len
    left = jnp.clip(lengths[:, None] - first_token[None, :], 0, block_len)
    filled = jnp.sum(jnp.where(matches, left[:, :, None], 0), axis=1)
    place = jnp.arange(2 * block_len, dtype=jnp.int32)
    limit = jnp.where(place % 2 == 0, place // 2, block_len)
    return (limit[None, None, :] < filled[:, :, None]).reshape(lengths.shape[0], -1)


def mamba_in(normed, layer, in_weight, xproj_weight, values):
    conv_weight, conv_bias, conv_state = values[:3]
    channels = in_weight.shape[3]
    both_proj = jnp.dot(
        normed,
        in_weight[layer].reshape(in_weight.shape[1], 2 * channels),
        preferred_element_type=jnp.float32,
    ).astype(jnp.bfloat16)
    inputs = both_proj[:, :channels]
    gate = jax.nn.silu(both_proj[:, channels:].astype(jnp.float32))
    window = jnp.concatenate([conv_state, inputs[:, None, :]], axis=1)
    conv_sum = (
        jnp.sum(window.astype(jnp.float32) * conv_weight[None], axis=1) + conv_bias[None, :]
    )
    signal = lax.optimization_barrier(jax.nn.silu(conv_sum).astype(jnp.bfloat16))
    x_terms = jnp.dot(signal, xproj_weight[layer], preferred_element_type=jnp.float32)
    return x_terms, signal, gate, window[:, 1:, :]


def mamba_out(mapped_vectors, signal, gate, layer, dt_weight, out_weight, values):
    dt_bias, decay, skip_gain, ssm_state = values[3:]
    low_rank = dt_weight.shape[1]
    state_size = decay.shape[0]
    dt_low = mapped_vectors[:, :low_rank].astype(jnp.bfloat16)
    b_in = mapped_vectors[:, low_rank : low_rank + state_size]
    c_out = mapped_vectors[:, low_rank + state_size :]
    dt_step = jax.nn.softplus(
        jnp.dot(dt_low, dt_weight[layer], preferred_element_type=jnp.float32) + dt_bias[None, :]
    )
    widened = signal.astype(jnp.float32)
    decay_rate = jnp.exp(-dt_step[:, None, :] * decay[None])
    fresh_state = decay_rate * ssm_state + (dt_step * widened)[:, None, :] * b_in[:, :, None]
    readout = jnp.sum(fresh_state * c_out[:, :, None], axis=1) + skip_gain[None, :] * widened
    gated_out = (readout * gate).astype(jnp.bfloat16)
    partial = jnp.dot(gated_out, out_weight[layer], preferred_element_type=jnp.float32)
    rows, dim = partial.shape
    parts = lax.axis_size(SEQ)
    blocks = partial.astype(WIRE).reshape(rows, parts, dim // parts).swapaxes(0, 1)
    return blocks, fresh_state


def block_sums(blocks):
    arrived = lax.all_to_all(blocks, SEQ, split_axis=0, concat_axis=0, tiled=True)
    return of_everyone(jnp.sum(arrived.astype(jnp.float32), axis=0), CHAN)


def local_attention(questions, kv_rows, in_use, inv_sqrt):
    requests, group_size, width = questions.shape
    tokens = kv_rows.shape[0]
    visible = in_use[:, None, :]
    scores = (
        jnp.dot(
            questions.reshape(requests * group_size, width),
            kv_rows.T,
            preferred_element_type=jnp.float32,
        )
        * inv_sqrt
    ).reshape(requests, group_size, tokens)
    scores = jnp.where(visible, scores, lowest_score)
    high, low = two_parts(jnp.max(scores, axis=2))
    weight = jnp.where(visible, jnp.exp(scores - (high + low)[..., None]), 0.0)
    total = jnp.sum(weight, axis=2)
    moved = jnp.roll(
        weight.astype(jnp.bfloat16).reshape(requests * group_size, tokens), 1, axis=1
    )
    mixed = jnp.dot(moved, kv_rows, preferred_element_type=jnp.float32)
    return high, low, total, mixed


def project_questions(stream_one, gain_block, asker_lookup_matrix, model_dim):
    requests = stream_one.shape[0]
    entries = asker_lookup_matrix.shape[2]
    widened = stream_one.astype(jnp.float32)
    high, low = two_parts(jnp.sum(widened * widened, axis=1))
    scaled = (widened * gain_block[None, :]).astype(jnp.bfloat16)
    terms = jnp.dot(scaled, asker_lookup_matrix[:, 0, :], preferred_element_type=jnp.float32)
    summed = of_everyone(
        jnp.concatenate([terms, high[:, None], low[:, None], jnp.zeros((requests, 126))], axis=1),
        SEQ,
    )
    inv_rms = lax.rsqrt((summed[:, entries] + summed[:, entries + 1]) / model_dim + norm_eps)
    return (summed[:, :entries] * inv_rms[:, None]).astype(jnp.bfloat16)


def attend(qkv, kv_rows, in_use, width):
    requests, entries = qkv.shape
    group_size = entries // width - 2
    rows = requests * group_size
    inv_sqrt = width ** (-0.5)
    questions = qkv[:, : group_size * width].reshape(requests, group_size, width)
    fresh_key = qkv[:, group_size * width : (group_size + 1) * width]
    fresh_value = qkv[:, (group_size + 1) * width :]
    fresh_score = (
        jnp.sum(
            questions.astype(jnp.float32) * fresh_key[:, None, :].astype(jnp.float32), axis=2
        )
        * inv_sqrt
    )
    high, low, total, mixed = local_attention(questions, kv_rows, in_use, inv_sqrt)
    notes = jnp.stack([high.reshape(rows), low.reshape(rows), total.reshape(rows)])
    notes = jnp.pad(notes, ((0, 5), (0, width - rows)))
    packed = jnp.concatenate([mixed, notes], axis=0).astype(WIRE)
    packed, fresh_score, fresh_value = lax.optimization_barrier(
        (packed, fresh_score, fresh_value.astype(jnp.float32))
    )
    arrived = copy_for_each(packed, SEQ).astype(jnp.float32)
    tops = (arrived[:, rows, :rows] + arrived[:, rows + 1, :rows]).reshape(
        -1, requests, group_size
    )
    totals = arrived[:, rows + 2, :rows].reshape(-1, requests, group_size)
    mixes = arrived[:, :rows].reshape(-1, requests, group_size, width)
    final_top = jnp.maximum(jnp.max(tops, axis=0), fresh_score)
    scale = jnp.exp(tops - final_top[None])
    fresh_weight = jnp.exp(fresh_score - final_top)
    denominator = jnp.sum(scale * totals, axis=0) + fresh_weight
    numerator = (
        jnp.sum(scale[..., None] * mixes, axis=0)
        + fresh_weight[..., None] * fresh_value[:, None, :]
    )
    attended = (numerator / denominator[..., None]).astype(jnp.bfloat16)
    return attended.reshape(requests, group_size * width)


def shards(
    hidden,
    norm_gain,
    in_weight,
    conv_weight,
    conv_bias,
    conv_state,
    xproj_weight,
    dt_weight,
    dt_bias,
    a_log,
    skip_gain,
    ssm_state,
    out_weight,
    asker_lookup_matrix,
    o_weight,
    kv_cache,
    lengths,
    page_table,
):
    requests, model_dim = hidden.shape
    block_cols = model_dim // lax.axis_size(SEQ)
    share_cols = block_cols // lax.axis_size(CHAN)
    small = (conv_weight, conv_bias, conv_state, dt_bias, a_log, skip_gain, ssm_state)
    pages_dev, block_len, pair, _, width = kv_cache.shape
    kv_rows = kv_cache.reshape(pages_dev * block_len * pair, width)
    first_col = lax.axis_index(SEQ) * block_cols
    values_first = layer_values(0, *small)
    terms, signal, gate, conv_first = mamba_in(
        normalize(hidden, norm_gain[0]), 0, in_weight, xproj_weight, values_first
    )
    side = (
        values_first,
        layer_values(1, *small),
        lax.dynamic_slice_in_dim(hidden, first_col, block_cols, 1),
        lax.dynamic_slice_in_dim(norm_gain[1], first_col, block_cols, 0),
        norm_gain[2].reshape(-1, 1, block_cols),
        rows_in_use(pages_dev, block_len, lengths, page_table),
        lax.axis_index(CHAN) * share_cols,
        signal,
        gate,
        conv_first,
    )
    copies = copy_for_each(terms.astype(WIRE), PLANE)
    copies, side = lax.optimization_barrier((copies, side))
    (
        values_first,
        values_second,
        own_block,
        gain_block,
        gain_second,
        in_use,
        first_share,
        signal,
        gate,
        conv_first,
    ) = side
    mapped_vectors = of_everyone(jnp.sum(copies.astype(jnp.float32), axis=0), LINE)
    blocks, state_first = mamba_out(
        mapped_vectors, signal, gate, 0, dt_weight, out_weight, values_first
    )
    blocks, state_first = lax.optimization_barrier((blocks, state_first))
    stream_one = (own_block.astype(jnp.float32) + block_sums(blocks)).astype(jnp.bfloat16)
    qkv = project_questions(stream_one, gain_block, asker_lookup_matrix, model_dim)
    attended = attend(qkv, kv_rows, in_use, width)
    attn_block = of_everyone(
        jnp.dot(attended, o_weight[0], preferred_element_type=jnp.float32), CHAN
    )
    stream_two = (stream_one.astype(jnp.float32) + attn_block).astype(jnp.bfloat16)
    whole_two = copy_for_each(stream_two, SEQ).astype(jnp.float32)
    inv_rms = lax.rsqrt(jnp.sum(whole_two * whole_two, axis=(0, 2)) / model_dim + norm_eps)
    normed = (whole_two * inv_rms[:, None] * gain_second).astype(jnp.bfloat16)
    terms, signal, gate, conv_second = mamba_in(
        normed.swapaxes(0, 1).reshape(requests, model_dim), 1, in_weight, xproj_weight, values_second
    )
    terms, gate, new_conv = lax.optimization_barrier(
        (terms, gate, jnp.stack([conv_first, conv_second]))
    )
    mapped_vectors = of_everyone(of_everyone(terms, PLANE), LINE)
    blocks, state_second = mamba_out(
        mapped_vectors, signal, gate, 1, dt_weight, out_weight, values_second
    )
    blocks, new_ssm = lax.optimization_barrier((blocks, jnp.stack([state_first, state_second])))
    added, qkv, first_share = lax.optimization_barrier((block_sums(blocks), qkv, first_share))
    newest_pair = qkv[:, -2 * width :].reshape(requests, 1, 2, width)
    out_block = (stream_two.astype(jnp.float32) + added).astype(jnp.bfloat16)
    hidden_out = lax.dynamic_slice_in_dim(out_block, first_share, share_cols, 1)
    return hidden_out, new_ssm, new_conv, newest_pair


def solution(mesh):
    split = Mesh(mesh.devices.reshape(8, 4, 4, 2), ALL)
    placed = (
        P(),
        P(),
        P(None, None, None, ALL),
        P(None, None, ALL),
        P(None, ALL),
        P(None, None, None, ALL),
        P(None, ALL, None),
        P(None, None, ALL),
        P(None, ALL),
        P(None, None, ALL),
        P(None, ALL),
        P(None, None, None, ALL),
        P(None, ALL, None),
        P(SEQ, CHAN, None),
        P(CHAN, None, SEQ),
        P(SEQ, None, None, CHAN, None),
        P(),
        P(),
    )
    return jax.shard_map(
        shards,
        mesh=split,
        in_specs=placed,
        out_specs=(
            P(None, ALL),
            P(None, None, None, ALL),
            P(None, None, None, ALL),
            P(None, CHAN, None, None),
        ),
        check_vma=False,
    )
```

```python
import functools

import jax
import jax.numpy as jnp
from jax import lax
from jax.experimental import pallas as pl
from jax.experimental.pallas import tpu as pltpu
from jax.sharding import Mesh
from jax.sharding import PartitionSpec as P

ALL = ("z", "x", "y", "core")
SEQ = ("z", "x")
SEQ_SUM = ("x", "z")
CHAN = ("y", "core")
CHAN_SUM = ("core", "y")
PLANE = ("x", "y")
LINE = ("core", "z")
WIRE = jnp.bfloat16
F32 = jnp.float32

norm_eps = 1e-06
lowest_score = -1e30


def exchange(copies, axes):
    return lax.all_to_all(copies, axes, split_axis=0, concat_axis=0, tiled=True)


def copied(x, axes):
    return jnp.broadcast_to(x, (lax.axis_size(axes), *x.shape))


def whole(shape):
    return pl.BlockSpec(shape, lambda _: (0,) * len(shape))


def layer_of(shape, layer):
    return pl.BlockSpec((1, *shape[1:]), lambda _: (layer,) + (0,) * (len(shape) - 1))


def local_call(body, inputs, outputs, scratch=(), aliases={}):
    def spec(shape, layer):
        if layer in ("far", "scalar"):
            return pl.BlockSpec(memory_space=pltpu.HBM if layer == "far" else pltpu.SMEM)
        return whole(shape) if layer is None else layer_of(shape, layer)

    return pl.pallas_call(
        body,
        grid=(1,),
        in_specs=[spec(x.shape, layer) for x, layer in inputs],
        out_specs=[spec(shape, layer) for shape, _, layer in outputs],
        out_shape=[jax.ShapeDtypeStruct(shape, dtype) for shape, dtype, _ in outputs],
        scratch_shapes=list(scratch),
        input_output_aliases=aliases,
        compiler_params=pltpu.CompilerParams(vmem_limit_bytes=12 * 1024 * 1024),
    )(*[x for x, _ in inputs])


def silu(x):
    return x * lax.logistic(x)


def added_up(ref):
    total = ref[0].astype(F32)
    for k in range(1, ref.shape[0]):
        total = total + ref[k].astype(F32)
    return total


def store_copies(ref, x):
    for k in range(ref.shape[0]):
        ref[k] = x


def against_rows(a, b):
    return lax.dot_general(a, b, (((1,), (1,)), ((), ())), preferred_element_type=F32)


def mamba_in_body(layer, *refs):
    refs = list(refs)
    stream_ref, gain_ref, in_ref, taps_ref, bias_ref, past_ref, xproj_ref = refs[:7]
    terms_ref, signal_ref, gate_ref, conv_ref, normed_ref, held_ref, done = refs[-7:]
    dim = normed_ref.shape[1]
    pieces = done.shape[0]
    piece = dim // pieces
    copies = [
        pltpu.make_async_copy(
            in_ref.at[layer, :, :, pl.ds(k * piece, piece)],
            held_ref.at[:, :, pl.ds(k * piece, piece)],
            done.at[k],
        )
        for k in range(pieces)
    ]
    for copy in copies:
        copy.start()
    gain_row = (0, None, 2)[2 * layer]
    if len(stream_ref.shape) == 2:
        x = stream_ref[...].astype(F32)
        inv_rms = lax.rsqrt(jnp.sum(x * x, axis=1, keepdims=True) / dim + norm_eps)
        normed_ref[...] = (x * inv_rms * gain_ref[gain_row : gain_row + 1, :]).astype(jnp.bfloat16)
    else:
        blocks, _, width = stream_ref.shape
        squares = jnp.zeros(stream_ref.shape[1:], F32)
        for k in range(blocks):
            x = stream_ref[k].astype(F32)
            squares = squares + x * x
        inv_rms = lax.rsqrt(jnp.sum(squares, axis=1, keepdims=True) / dim + norm_eps)
        for k in range(blocks):
            cols = slice(k * width, (k + 1) * width)
            normed_ref[:, cols] = (
                stream_ref[k].astype(F32) * inv_rms * gain_ref[gain_row : gain_row + 1, cols]
            ).astype(jnp.bfloat16)
    inputs = jnp.zeros(signal_ref.shape, F32)
    gates = jnp.zeros(signal_ref.shape, F32)
    for k, copy in enumerate(copies):
        copy.wait()
        cols = slice(k * piece, (k + 1) * piece)
        normed = normed_ref[:, cols]
        inputs = inputs + against_rows(normed, held_ref[0, :, cols])
        gates = gates + against_rows(normed, held_ref[1, :, cols])
    inputs = inputs.astype(jnp.bfloat16)
    gates = gates.astype(jnp.bfloat16)
    taps = taps_ref[0]
    conv_sum = inputs.astype(F32) * taps[3:4]
    for k in range(3):
        conv_sum = conv_sum + past_ref[0, k].astype(F32) * taps[k : k + 1]
    signal = silu(conv_sum + bias_ref[layer : layer + 1, :]).astype(jnp.bfloat16)
    terms = jnp.dot(signal, xproj_ref[0], preferred_element_type=F32)
    store_copies(terms_ref, terms.astype(WIRE))
    signal_ref[...] = signal.astype(F32)
    gate_ref[...] = silu(gates.astype(F32))
    conv_ref[0, 0] = past_ref[0, 1]
    conv_ref[0, 1] = past_ref[0, 2]
    conv_ref[0, 2] = inputs


def mamba_in(stream, layer, norm_gain, in_rows, conv_weight, conv_bias, past, xproj_weight, conv_so_far):
    requests = past.shape[2]
    channels = past.shape[3]
    inputs = [
        (stream, None),
        (norm_gain, None),
        (in_rows, "far"),
        (conv_weight, layer),
        (conv_bias, None),
        (past, layer),
        (xproj_weight, layer),
    ]
    aliases = {}
    if conv_so_far is not None:
        aliases = {len(inputs): 3}
        inputs.append((conv_so_far, "far"))
    terms, signal, gate, conv = local_call(
        functools.partial(mamba_in_body, layer),
        inputs,
        [
            ((lax.axis_size(PLANE), requests, xproj_weight.shape[2]), WIRE, None),
            ((requests, channels), F32, None),
            ((requests, channels), F32, None),
            (past.shape, jnp.bfloat16, layer),
        ],
        [
            pltpu.VMEM((requests, in_rows.shape[3]), jnp.bfloat16),
            pltpu.VMEM(in_rows.shape[1:], jnp.bfloat16),
            pltpu.SemaphoreType.DMA((4,)),
        ],
        aliases,
    )
    return terms, signal, gate, conv


def mamba_out_body(layer, order, *refs):
    arrived_ref, signal_ref, gate_ref, dt_ref, bias_ref, decay_ref, skip_ref, state_ref, out_ref = (
        refs[:9]
    )
    blocks_ref, fresh_ref = refs[-2:]
    mapped = added_up(arrived_ref)
    low_rank = dt_ref.shape[2]
    states = decay_ref.shape[1]
    low = mapped[:, :low_rank].astype(jnp.bfloat16)
    raw = against_rows(low, dt_ref[0]) + bias_ref[layer : layer + 1, :]
    step = jnp.maximum(raw, 0.0) + jnp.log1p(jnp.exp(-jnp.abs(raw)))
    signal = signal_ref[...]
    pushed = step * signal
    rates = jnp.exp(decay_ref[0])
    rest = mapped[:, low_rank:]
    eye = lax.broadcasted_iota(jnp.int32, (states, states), 0) == lax.broadcasted_iota(
        jnp.int32, (states, states), 1
    )

    def column(row):
        return jnp.sum(jnp.where(eye, row, 0.0), axis=1, keepdims=True)

    readouts = []
    for b in range(mapped.shape[0]):
        b_in = column(rest[b : b + 1, :states])
        c_out = column(rest[b : b + 1, states : 2 * states])
        fresh = (
            jnp.exp(-step[b : b + 1] * rates) * state_ref[0, b] + pushed[b : b + 1] * b_in
        )
        fresh_ref[0, b] = fresh
        readouts.append(jnp.sum(fresh * c_out, axis=0, keepdims=True))
    readout = jnp.concatenate(readouts, axis=0) + skip_ref[layer : layer + 1, :] * signal
    gated = (readout * gate_ref[...]).astype(jnp.bfloat16)
    width = blocks_ref.shape[2]
    for place, block in enumerate(order):
        blocks_ref[place] = jnp.dot(
            gated,
            out_ref[0, :, block * width : (block + 1) * width],
            preferred_element_type=F32,
        ).astype(WIRE)


def mamba_out(arrived, signal, gate, layer, dt_rows, dt_bias, a_log, skip_gain, ssm_state, out_weight, so_far):
    far, near = (lax.axis_size(axis) for axis in SEQ_SUM)
    order = [k * far + j for j in range(far) for k in range(near)]
    inputs = [
        (arrived, None),
        (signal, None),
        (gate, None),
        (dt_rows, layer),
        (dt_bias, None),
        (a_log, layer),
        (skip_gain, None),
        (ssm_state, layer),
        (out_weight, layer),
    ]
    aliases = {}
    if so_far is not None:
        aliases = {len(inputs): 1}
        inputs.append((so_far, "far"))
    blocks, fresh = local_call(
        functools.partial(mamba_out_body, layer, order),
        inputs,
        [
            ((far * near, signal.shape[0], out_weight.shape[2] // (far * near)), WIRE, None),
            (ssm_state.shape, F32, layer),
        ],
        (),
        aliases,
    )
    arrived = exchange(blocks, SEQ_SUM)
    own = jnp.sum(arrived.astype(F32), axis=0).astype(WIRE)
    return exchange(copied(own, CHAN_SUM), CHAN_SUM), fresh


def two_parts(x):
    high = x.astype(WIRE).astype(F32)
    return high, x - high


def questions_body(arrived_ref, hidden_ref, gain_ref, matrix_ref, stream_ref, terms_ref):
    width = stream_ref.shape[1]
    first = pl.multiple_of(seq_index() * width, width)
    stream = (hidden_ref[:, pl.ds(first, width)].astype(F32) + added_up(arrived_ref)).astype(
        jnp.bfloat16
    )
    stream_ref[...] = stream
    wide = stream.astype(F32)
    high, low = two_parts(jnp.sum(wide * wide, axis=1, keepdims=True))
    scaled = (wide * gain_ref[1:2, pl.ds(first, width)]).astype(jnp.bfloat16)
    terms = jnp.dot(scaled, matrix_ref[...], preferred_element_type=F32)
    lane = lax.broadcasted_iota(jnp.int32, (stream.shape[0], 128), 1)
    notes = jnp.where(lane == 0, high, jnp.where(lane == 1, low, 0.0))
    entries = terms.shape[1]
    for k in range(terms_ref.shape[0]):
        terms_ref[k, :, :entries] = terms.astype(WIRE)
        terms_ref[k, :, entries:] = notes.astype(WIRE)


def seq_index():
    return lax.axis_index("z") * lax.axis_size("x") + lax.axis_index("x")


def flip(x):
    n = max(x.shape)
    eye = lax.broadcasted_iota(jnp.int32, (n, n), 0) == lax.broadcasted_iota(jnp.int32, (n, n), 1)
    return jnp.sum(jnp.where(eye, x, 0.0), axis=x.shape.index(n), keepdims=True)


def store_part(out_ref, top, total, mixed):
    rows, width = mixed.shape
    high, low = two_parts(top)
    pad = jnp.zeros((1, width - rows), F32)
    notes = [jnp.concatenate([v, pad], axis=1) for v in (high, low, total)]
    notes = jnp.concatenate([*notes, jnp.zeros((out_ref.shape[1] - rows - 3, width), F32)], axis=0)
    for k in range(out_ref.shape[0]):
        out_ref[k, :rows, :] = mixed.astype(WIRE)
        out_ref[k, rows:, :] = notes.astype(WIRE)


def merged(arrived_ref):
    parts, stored, _ = arrived_ref.shape
    rows = stored - 8
    notes = [arrived_ref[k, rows:, :].astype(F32) for k in range(parts)]
    tops = [v[0:1, :rows] + v[1:2, :rows] for v in notes]
    top = tops[0]
    for v in tops[1:]:
        top = jnp.maximum(top, v)
    total = jnp.zeros_like(top)
    mixed = jnp.zeros((rows, arrived_ref.shape[2]), F32)
    for k in range(parts):
        scale = jnp.exp(tops[k] - top)
        total = total + scale * notes[k][2:3, :rows]
        mixed = mixed + flip(scale) * arrived_ref[k, :rows, :].astype(F32)
    return top, total, mixed


def attention_body(
    arrived_ref, kv_ref, lengths_ref, table_ref, part_ref, pair_ref, questions_ref, scores_ref, *, block_len, dim
):
    summed = added_up(arrived_ref)
    requests = summed.shape[0]
    width = kv_ref.shape[1]
    entries = summed.shape[1] - 128
    group_size = entries // width - 2
    rows = requests * group_size
    tokens = kv_ref.shape[0]
    chunk = 2 * block_len
    inv_rms = lax.rsqrt((summed[:, entries : entries + 1] + summed[:, entries + 1 : entries + 2]) / dim + norm_eps)
    qkv = (summed[:, :entries] * inv_rms).astype(jnp.bfloat16)
    fresh = qkv[:, group_size * width :]
    fresh = fresh.astype(F32)
    pair_ref[...] = fresh
    fresh_scores = []
    for g in range(group_size):
        one = qkv[:, g * width : (g + 1) * width]
        questions_ref[g * requests : (g + 1) * requests, :] = one.astype(F32)
        fresh_scores.append(jnp.sum(one.astype(F32) * fresh[:, :width], axis=1, keepdims=True))
    questions = questions_ref[...].astype(jnp.bfloat16)
    inv_sqrt = width ** (-0.5)
    is_first = seq_index() == 0
    fresh_score = jnp.where(is_first, jnp.concatenate(fresh_scores, axis=0) * inv_sqrt, lowest_score)
    first_slot = seq_index() * (tokens // chunk)
    table = table_ref[...]
    row = lax.broadcasted_iota(jnp.int32, table.shape, 0)
    lengths = jnp.zeros(table.shape, jnp.int32)
    for b in range(requests):
        lengths = jnp.where(row == b, lengths_ref[b], lengths)
    left = jnp.clip(
        lengths - lax.broadcasted_iota(jnp.int32, table.shape, 1) * block_len, 0, block_len
    )
    place = lax.broadcasted_iota(jnp.int32, (requests, chunk), 1)
    limit = jnp.where(place % 2 == 0, place // 2, block_len)
    top = fresh_score
    hidden_from = []
    for k in range(tokens // chunk):
        filled = jnp.sum(jnp.where(table == first_slot + k, left, 0), axis=1, keepdims=True)
        visible = jnp.concatenate([(limit < filled).astype(F32)] * group_size, axis=0) > 0.5
        hidden_from.append(visible)
        scores = against_rows(questions, kv_ref[k * chunk : (k + 1) * chunk, :]) * inv_sqrt
        scores = jnp.where(visible, scores, lowest_score)
        scores_ref[:, k * chunk : (k + 1) * chunk] = scores
        top = jnp.maximum(top, jnp.max(scores, axis=1, keepdims=True))
    high, low = two_parts(top)
    top = high + low.astype(WIRE).astype(F32)
    weight = jnp.where(is_first, jnp.exp(fresh_score - top), 0.0)
    total = weight
    values = jnp.concatenate([fresh[:, width:]] * group_size, axis=0)
    mixed = weight * values
    for k in range(tokens // chunk):
        weight = jnp.where(
            hidden_from[k], jnp.exp(scores_ref[:, k * chunk : (k + 1) * chunk] - top), 0.0
        )
        total = total + jnp.sum(weight, axis=1, keepdims=True)
        moved = pltpu.roll(weight, 1, 1).astype(jnp.bfloat16)
        mixed = mixed + jnp.dot(moved, kv_ref[k * chunk : (k + 1) * chunk, :], preferred_element_type=F32)
    store_part(part_ref, flip(top), flip(total), mixed)


def merge_body(arrived_ref, part_ref):
    top, total, mixed = merged(arrived_ref)
    store_part(part_ref, top, total, mixed)


def attention_out_body(arrived_ref, weight_ref, sums_ref):
    _, total, mixed = merged(arrived_ref)
    attended = (mixed / flip(total)).astype(jnp.bfloat16)
    requests = sums_ref.shape[1]
    width = attended.shape[1]
    result = jnp.zeros(sums_ref.shape[1:], F32)
    for g in range(attended.shape[0] // requests):
        result = result + jnp.dot(
            attended[g * requests : (g + 1) * requests],
            weight_ref[g * width : (g + 1) * width, :],
            preferred_element_type=F32,
        )
    store_copies(sums_ref, result.astype(WIRE))


def last_body(arrived_ref, stream_ref, fresh_ref, out_ref, pair_ref):
    head = pair_ref.shape[3]
    for b in range(pair_ref.shape[0]):
        pair_ref[b, 0] = jnp.concatenate(
            [fresh_ref[b : b + 1, :head], fresh_ref[b : b + 1, head:]], axis=0
        ).astype(jnp.bfloat16)
    result = (stream_ref[...].astype(F32) + added_up(arrived_ref)).astype(jnp.bfloat16)
    place = lax.axis_index("y") * lax.axis_size("core") + lax.axis_index("core")
    width = out_ref.shape[1]
    result = result.astype(F32)
    own = result[:, :width]
    for k in range(1, result.shape[1] // width):
        own = jnp.where(place == k, result[:, k * width : (k + 1) * width], own)
    out_ref[...] = own.astype(jnp.bfloat16)


def shards(
    hidden,
    norm_gain,
    in_weight,
    conv_weight,
    conv_bias,
    conv_state,
    xproj_weight,
    dt_weight,
    dt_bias,
    a_log,
    skip_gain,
    ssm_state,
    out_weight,
    asker_lookup_matrix,
    o_weight,
    kv_cache,
    lengths,
    page_table,
):
    requests, model_dim = hidden.shape
    block_cols = model_dim // lax.axis_size(SEQ)
    share_cols = block_cols // lax.axis_size(CHAN)
    pages_dev, block_len, pair, _, width = kv_cache.shape
    entries = asker_lookup_matrix.shape[2]
    rows = requests * (entries // width - 2)
    in_rows = pltpu.with_memory_space_constraint(in_weight.transpose(0, 2, 3, 1), pltpu.HBM)
    dt_rows = dt_weight.transpose(0, 2, 1)
    past = conv_state.transpose(0, 2, 1, 3)
    kv_rows = kv_cache.reshape(pages_dev * block_len * pair, width)
    conv_args = (conv_weight, conv_bias, past, xproj_weight)
    state_args = (dt_rows, dt_bias, a_log, skip_gain, ssm_state, out_weight)

    def sums_of_proj(terms):
        own = jnp.sum(exchange(terms, PLANE).astype(F32), axis=0).astype(WIRE)
        return exchange(copied(own, LINE), LINE)

    terms, signal, gate, new_conv = mamba_in(hidden, 0, norm_gain, in_rows, *conv_args, None)
    arrived, new_ssm = mamba_out(sums_of_proj(terms), signal, gate, 0, *state_args, None)
    stream_one, terms = local_call(
        questions_body,
        [
            (arrived, None),
            (hidden, None),
            (norm_gain, None),
            (asker_lookup_matrix.reshape(block_cols, entries), None),
        ],
        [
            ((requests, block_cols), jnp.bfloat16, None),
            ((lax.axis_size("x"), requests, entries + 128), WIRE, None),
        ],
    )
    own = jnp.sum(exchange(terms, "x").astype(F32), axis=0).astype(WIRE)
    part, fresh = local_call(
        functools.partial(attention_body, block_len=block_len, dim=model_dim),
        [
            (exchange(copied(own, "z"), "z"), None),
            (kv_rows, None),
            (lengths, "scalar"),
            (page_table, None),
        ],
        [
            ((lax.axis_size("x"), rows + 8, width), WIRE, None),
            ((requests, 2 * width), F32, None),
        ],
        [pltpu.VMEM((rows, width), F32), pltpu.VMEM((rows, kv_rows.shape[0]), F32)],
    )
    (part,) = local_call(
        merge_body,
        [(exchange(part, "x"), None)],
        [((lax.axis_size("z"), rows + 8, width), WIRE, None)],
    )
    (sums,) = local_call(
        attention_out_body,
        [(exchange(part, "z"), None), (o_weight[0], None)],
        [((lax.axis_size(CHAN), requests, block_cols), WIRE, None)],
    )
    added = jnp.sum(exchange(sums, CHAN_SUM).astype(F32), axis=0)
    stream_two = (stream_one.astype(F32) + added).astype(jnp.bfloat16)
    terms, signal, gate, new_conv = mamba_in(
        exchange(copied(stream_two, SEQ), SEQ), 1, norm_gain, in_rows, *conv_args, new_conv
    )
    arrived, new_ssm = mamba_out(sums_of_proj(terms), signal, gate, 1, *state_args, new_ssm)
    hidden_out, newest_pair = local_call(
        last_body,
        [(arrived, None), (stream_two, None), (fresh, None)],
        [
            ((requests, share_cols), jnp.bfloat16, None),
            ((requests, 1, 2, width), jnp.bfloat16, None),
        ],
    )
    return hidden_out, new_ssm, new_conv.transpose(0, 2, 1, 3), newest_pair


def solution(mesh):
    split = Mesh(mesh.devices.reshape(8, 4, 4, 2), ALL)
    placed = (
        P(),
        P(),
        P(None, None, None, ALL),
        P(None, None, ALL),
        P(None, ALL),
        P(None, None, None, ALL),
        P(None, ALL, None),
        P(None, None, ALL),
        P(None, ALL),
        P(None, None, ALL),
        P(None, ALL),
        P(None, None, None, ALL),
        P(None, ALL, None),
        P(SEQ, CHAN, None),
        P(CHAN, None, SEQ),
        P(SEQ, None, None, CHAN, None),
        P(),
        P(),
    )
    return jax.shard_map(
        shards,
        mesh=split,
        in_specs=placed,
        out_specs=(
            P(None, ALL),
            P(None, None, None, ALL),
            P(None, None, None, ALL),
            P(None, CHAN, None, None),
        ),
        check_vma=False,
    )
```

```python
import functools

import jax
import jax.numpy as jnp
from jax import lax
from jax.experimental import pallas as pl
from jax.experimental.pallas import tpu as pltpu
from jax.sharding import Mesh
from jax.sharding import PartitionSpec as P

ALL = ("z", "x", "y", "core")
SEQ = ("z", "x")
SEQ_SUM = ("x", "z")
CHAN = ("y", "core")
CHAN_SUM = ("core", "y")
PLANE = ("x", "y")
LINE = ("core", "z")
WIRE = jnp.bfloat16
F32 = jnp.float32

norm_eps = 1e-06
lowest_score = -1e30


def exchange(copies, axes):
    return lax.all_to_all(copies, axes, split_axis=0, concat_axis=0, tiled=True)


def copied(x, axes):
    return jnp.broadcast_to(x, (lax.axis_size(axes), *x.shape))


def whole(shape):
    return pl.BlockSpec(shape, lambda _: (0,) * len(shape))


def layer_of(shape, layer):
    return pl.BlockSpec((1, *shape[1:]), lambda _: (layer,) + (0,) * (len(shape) - 1))


def far(x):
    return pltpu.with_memory_space_constraint(x, pltpu.HBM)


def local_call(body, inputs, outputs, scratch=(), aliases={}):
    def spec(shape, layer):
        if layer in ("far", "scalar"):
            return pl.BlockSpec(memory_space=pltpu.HBM if layer == "far" else pltpu.SMEM)
        return whole(shape) if layer is None else layer_of(shape, layer)

    return pl.pallas_call(
        body,
        grid=(1,),
        in_specs=[spec(x.shape, layer) for x, layer in inputs],
        out_specs=[spec(shape, layer) for shape, _, layer in outputs],
        out_shape=[jax.ShapeDtypeStruct(shape, dtype) for shape, dtype, _ in outputs],
        scratch_shapes=list(scratch),
        input_output_aliases=aliases,
        compiler_params=pltpu.CompilerParams(vmem_limit_bytes=12 * 1024 * 1024),
    )(*[x for x, _ in inputs])


def silu(x):
    return x * lax.logistic(x)


def added_up(ref):
    total = ref[0].astype(F32)
    for k in range(1, ref.shape[0]):
        total = total + ref[k].astype(F32)
    return total


def store_copies(ref, x):
    for k in range(ref.shape[0]):
        ref[k] = x


def against_rows(a, b):
    return lax.dot_general(a, b, (((1,), (1,)), ((), ())), preferred_element_type=F32)


def mamba_in_body(layer, *refs):
    stream_ref, gain_ref, in_ref, taps_ref, bias_ref, past_ref, xproj_ref = refs[:7]
    normed_ref, held_ref, done = refs[-3:]
    terms_ref, signal_ref, gate_ref, conv_ref = refs[7:11] if layer == 0 else refs[8:12]
    dim = normed_ref.shape[1]
    pieces = done.shape[0]
    piece = dim // pieces
    copies = [
        pltpu.make_async_copy(
            in_ref.at[layer, :, :, pl.ds(k * piece, piece)],
            held_ref.at[:, :, pl.ds(k * piece, piece)],
            done.at[k],
        )
        for k in range(pieces)
    ]
    for copy in copies:
        copy.start()
    if layer == 0:
        own_ref, own_gain_ref = refs[11:13]
        width = own_ref.shape[1]
        first = pl.multiple_of(seq_index() * width, width)
        own_ref[...] = stream_ref[:, pl.ds(first, width)]
        own_gain_ref[...] = gain_ref[1:2, pl.ds(first, width)]
    gain_row = (0, None, 2)[2 * layer]
    if len(stream_ref.shape) == 2:
        x = stream_ref[...].astype(F32)
        inv_rms = lax.rsqrt(jnp.sum(x * x, axis=1, keepdims=True) / dim + norm_eps)
        normed_ref[...] = (x * inv_rms * gain_ref[gain_row : gain_row + 1, :]).astype(jnp.bfloat16)
    else:
        blocks, _, width = stream_ref.shape
        squares = jnp.zeros(stream_ref.shape[1:], F32)
        for k in range(blocks):
            x = stream_ref[k].astype(F32)
            squares = squares + x * x
        inv_rms = lax.rsqrt(jnp.sum(squares, axis=1, keepdims=True) / dim + norm_eps)
        for k in range(blocks):
            cols = slice(k * width, (k + 1) * width)
            normed_ref[:, cols] = (
                stream_ref[k].astype(F32) * inv_rms * gain_ref[gain_row : gain_row + 1, cols]
            ).astype(jnp.bfloat16)
    inputs = jnp.zeros(signal_ref.shape, F32)
    gates = jnp.zeros(signal_ref.shape, F32)
    for k, copy in enumerate(copies):
        copy.wait()
        cols = slice(k * piece, (k + 1) * piece)
        normed = normed_ref[:, cols]
        inputs = inputs + against_rows(normed, held_ref[0, :, cols])
        gates = gates + against_rows(normed, held_ref[1, :, cols])
    inputs = inputs.astype(jnp.bfloat16)
    gates = gates.astype(jnp.bfloat16)
    taps = taps_ref[0]
    conv_sum = inputs.astype(F32) * taps[3:4]
    for k in range(3):
        conv_sum = conv_sum + past_ref[0, k].astype(F32) * taps[k : k + 1]
    signal = silu(conv_sum + bias_ref[layer : layer + 1, :]).astype(jnp.bfloat16)
    terms = jnp.dot(signal, xproj_ref[0], preferred_element_type=F32)
    store_copies(terms_ref, terms.astype(WIRE))
    signal_ref[...] = signal.astype(F32)
    gate_ref[...] = silu(gates.astype(F32))
    conv_ref[0, 0] = past_ref[0, 1]
    conv_ref[0, 1] = past_ref[0, 2]
    conv_ref[0, 2] = inputs


def mamba_in(
    stream, layer, norm_gain, in_rows, conv_weight, conv_bias, past, xproj_weight, conv_so_far
):
    requests = past.shape[2]
    channels = past.shape[3]
    inputs = [
        (stream, None),
        (norm_gain, None),
        (in_rows, "far"),
        (conv_weight, layer),
        (conv_bias, None),
        (past, layer),
        (xproj_weight, layer),
    ]
    aliases = {}
    if conv_so_far is not None:
        aliases = {len(inputs): 3}
        inputs.append((conv_so_far, "far"))
    extra = []
    if layer == 0:
        width = stream.shape[1] // lax.axis_size(SEQ)
        extra = [((requests, width), jnp.bfloat16, None), ((1, width), F32, None)]
    return local_call(
        functools.partial(mamba_in_body, layer),
        inputs,
        [
            ((lax.axis_size(PLANE), requests, xproj_weight.shape[2]), WIRE, None),
            ((requests, channels), F32, None),
            ((requests, channels), F32, None),
            (past.shape, jnp.bfloat16, layer),
            *extra,
        ],
        [
            pltpu.VMEM((requests, in_rows.shape[3]), jnp.bfloat16),
            pltpu.VMEM(in_rows.shape[1:], jnp.bfloat16),
            pltpu.SemaphoreType.DMA((4,)),
        ],
        aliases,
    )


def mamba_out_body(layer, order, *refs):
    arrived_ref, signal_ref, gate_ref, dt_ref, bias_ref, decay_ref, skip_ref, state_ref, out_ref = (
        refs[:9]
    )
    blocks_ref, fresh_ref, held_ref, done = refs[-4:]
    pieces = done.shape[0]
    piece = held_ref.shape[1] // pieces
    copies = [
        pltpu.make_async_copy(
            out_ref.at[layer, :, pl.ds(k * piece, piece)],
            held_ref.at[:, pl.ds(k * piece, piece)],
            done.at[k],
        )
        for k in range(pieces)
    ]
    for copy in copies:
        copy.start()
    mapped = added_up(arrived_ref)
    low_rank = dt_ref.shape[2]
    states = decay_ref.shape[1]
    low = mapped[:, :low_rank].astype(jnp.bfloat16)
    raw = against_rows(low, dt_ref[0]) + bias_ref[layer : layer + 1, :]
    step = jnp.maximum(raw, 0.0) + jnp.log1p(jnp.exp(-jnp.abs(raw)))
    signal = signal_ref[...]
    pushed = step * signal
    rates = jnp.exp(decay_ref[0])
    rest = mapped[:, low_rank:]
    eye = lax.broadcasted_iota(jnp.int32, (states, states), 0) == lax.broadcasted_iota(
        jnp.int32, (states, states), 1
    )

    def column(row):
        return jnp.sum(jnp.where(eye, row, 0.0), axis=1, keepdims=True)

    readouts = []
    for b in range(mapped.shape[0]):
        b_in = column(rest[b : b + 1, :states])
        c_out = column(rest[b : b + 1, states : 2 * states])
        fresh = (
            jnp.exp(-step[b : b + 1] * rates) * state_ref[0, b] + pushed[b : b + 1] * b_in
        )
        fresh_ref[0, b] = fresh
        readouts.append(jnp.sum(fresh * c_out, axis=0, keepdims=True))
    readout = jnp.concatenate(readouts, axis=0) + skip_ref[layer : layer + 1, :] * signal
    gated = (readout * gate_ref[...]).astype(jnp.bfloat16)
    width = blocks_ref.shape[2]
    for place, block in sorted(enumerate(order), key=lambda pair: pair[1]):
        if block * width % piece == 0:
            copies[block * width // piece].wait()
        blocks_ref[place] = jnp.dot(
            gated,
            held_ref[:, block * width : (block + 1) * width],
            preferred_element_type=F32,
        ).astype(WIRE)


def mamba_out(
    arrived, signal, gate, layer, dt_rows, ssm_state, dt_bias, a_log, skip_gain, out_weight, so_far
):
    wide, deep = (lax.axis_size(axis) for axis in SEQ_SUM)
    order = [k * wide + j for j in range(wide) for k in range(deep)]
    inputs = [
        (arrived, None),
        (signal, None),
        (gate, None),
        (dt_rows, min(layer, dt_rows.shape[0] - 1)),
        (dt_bias, None),
        (a_log, layer),
        (skip_gain, None),
        (ssm_state, min(layer, ssm_state.shape[0] - 1)),
        (far(out_weight), "far"),
    ]
    aliases = {}
    if so_far is not None:
        aliases = {len(inputs): 1}
        inputs.append((so_far, "far"))
    blocks, fresh = local_call(
        functools.partial(mamba_out_body, layer, order),
        inputs,
        [
            ((wide * deep, signal.shape[0], out_weight.shape[2] // (wide * deep)), WIRE, None),
            ((a_log.shape[0], *ssm_state.shape[1:]), F32, layer),
        ],
        [pltpu.VMEM(out_weight.shape[1:], jnp.bfloat16), pltpu.SemaphoreType.DMA((2,))],
        aliases,
    )
    arrived = exchange(blocks, SEQ_SUM)
    own = jnp.sum(arrived.astype(F32), axis=0).astype(WIRE)
    return exchange(copied(own, CHAN_SUM), CHAN_SUM), fresh


def two_parts(x):
    high = x.astype(WIRE).astype(F32)
    return high, x - high


def questions_body(arrived_ref, hidden_ref, gain_ref, matrix_ref, stream_ref, terms_ref):
    stream = (hidden_ref[...].astype(F32) + added_up(arrived_ref)).astype(jnp.bfloat16)
    stream_ref[...] = stream
    wide = stream.astype(F32)
    high, low = two_parts(jnp.sum(wide * wide, axis=1, keepdims=True))
    scaled = (wide * gain_ref[...]).astype(jnp.bfloat16)
    terms = jnp.dot(scaled, matrix_ref[...], preferred_element_type=F32)
    lane = lax.broadcasted_iota(jnp.int32, (stream.shape[0], 128), 1)
    notes = jnp.where(lane == 0, high, jnp.where(lane == 1, low, 0.0))
    entries = terms.shape[1]
    for k in range(terms_ref.shape[0]):
        terms_ref[k, :, :entries] = terms.astype(WIRE)
        terms_ref[k, :, entries:] = notes.astype(WIRE)


def seq_index():
    return lax.axis_index("z") * lax.axis_size("x") + lax.axis_index("x")


def flip(x):
    n = max(x.shape)
    eye = lax.broadcasted_iota(jnp.int32, (n, n), 0) == lax.broadcasted_iota(jnp.int32, (n, n), 1)
    return jnp.sum(jnp.where(eye, x, 0.0), axis=x.shape.index(n), keepdims=True)


def store_part(out_ref, top, total, mixed):
    rows, width = mixed.shape
    high, low = two_parts(top)
    pad = jnp.zeros((1, width - rows), F32)
    notes = [jnp.concatenate([v, pad], axis=1) for v in (high, low, total)]
    notes = jnp.concatenate([*notes, jnp.zeros((out_ref.shape[1] - rows - 3, width), F32)], axis=0)
    for k in range(out_ref.shape[0]):
        out_ref[k, :rows, :] = mixed.astype(WIRE)
        out_ref[k, rows:, :] = notes.astype(WIRE)


def merged(arrived_ref):
    parts, stored, _ = arrived_ref.shape
    rows = stored - 8
    notes = [arrived_ref[k, rows:, :].astype(F32) for k in range(parts)]
    tops = [v[0:1, :rows] + v[1:2, :rows] for v in notes]
    top = tops[0]
    for v in tops[1:]:
        top = jnp.maximum(top, v)
    total = jnp.zeros_like(top)
    mixed = jnp.zeros((rows, arrived_ref.shape[2]), F32)
    for k in range(parts):
        scale = jnp.exp(tops[k] - top)
        total = total + scale * notes[k][2:3, :rows]
        mixed = mixed + flip(scale) * arrived_ref[k, :rows, :].astype(F32)
    return top, total, mixed


def attention_body(
    arrived_ref, kv_ref, lengths_ref, table_ref, part_ref, pair_ref, questions_ref, scores_ref, *, block_len, dim
):
    summed = added_up(arrived_ref)
    requests = summed.shape[0]
    width = kv_ref.shape[1]
    entries = summed.shape[1] - 128
    group_size = entries // width - 2
    rows = requests * group_size
    tokens = kv_ref.shape[0]
    chunk = 2 * block_len
    inv_rms = lax.rsqrt((summed[:, entries : entries + 1] + summed[:, entries + 1 : entries + 2]) / dim + norm_eps)
    qkv = (summed[:, :entries] * inv_rms).astype(jnp.bfloat16)
    fresh = qkv[:, group_size * width :]
    fresh = fresh.astype(F32)
    pair_ref[...] = fresh
    fresh_scores = []
    for g in range(group_size):
        one = qkv[:, g * width : (g + 1) * width]
        questions_ref[g * requests : (g + 1) * requests, :] = one.astype(F32)
        fresh_scores.append(jnp.sum(one.astype(F32) * fresh[:, :width], axis=1, keepdims=True))
    questions = questions_ref[...].astype(jnp.bfloat16)
    inv_sqrt = width ** (-0.5)
    is_first = seq_index() == 0
    fresh_score = jnp.where(is_first, jnp.concatenate(fresh_scores, axis=0) * inv_sqrt, lowest_score)
    first_slot = seq_index() * (tokens // chunk)
    table = table_ref[...]
    row = lax.broadcasted_iota(jnp.int32, table.shape, 0)
    lengths = jnp.zeros(table.shape, jnp.int32)
    for b in range(requests):
        lengths = jnp.where(row == b, lengths_ref[b], lengths)
    left = jnp.clip(
        lengths - lax.broadcasted_iota(jnp.int32, table.shape, 1) * block_len, 0, block_len
    )
    place = lax.broadcasted_iota(jnp.int32, (requests, chunk), 1)
    limit = jnp.where(place % 2 == 0, place // 2, block_len)
    top = fresh_score
    hidden_from = []
    for k in range(tokens // chunk):
        filled = jnp.sum(jnp.where(table == first_slot + k, left, 0), axis=1, keepdims=True)
        visible = jnp.concatenate([(limit < filled).astype(F32)] * group_size, axis=0) > 0.5
        hidden_from.append(visible)
        scores = against_rows(questions, kv_ref[k * chunk : (k + 1) * chunk, :]) * inv_sqrt
        scores = jnp.where(visible, scores, lowest_score)
        scores_ref[:, k * chunk : (k + 1) * chunk] = scores
        top = jnp.maximum(top, jnp.max(scores, axis=1, keepdims=True))
    high, low = two_parts(top)
    top = high + low.astype(WIRE).astype(F32)
    weight = jnp.where(is_first, jnp.exp(fresh_score - top), 0.0)
    total = weight
    values = jnp.concatenate([fresh[:, width:]] * group_size, axis=0)
    mixed = weight * values
    for k in range(tokens // chunk):
        weight = jnp.where(
            hidden_from[k], jnp.exp(scores_ref[:, k * chunk : (k + 1) * chunk] - top), 0.0
        )
        total = total + jnp.sum(weight, axis=1, keepdims=True)
        moved = pltpu.roll(weight, 1, 1).astype(jnp.bfloat16)
        mixed = mixed + jnp.dot(moved, kv_ref[k * chunk : (k + 1) * chunk, :], preferred_element_type=F32)
    store_part(part_ref, flip(top), flip(total), mixed)


def merge_body(arrived_ref, part_ref):
    top, total, mixed = merged(arrived_ref)
    store_part(part_ref, top, total, mixed)


def attention_out_body(arrived_ref, weight_ref, sums_ref):
    _, total, mixed = merged(arrived_ref)
    attended = (mixed / flip(total)).astype(jnp.bfloat16)
    requests = sums_ref.shape[1]
    width = attended.shape[1]
    result = jnp.zeros(sums_ref.shape[1:], F32)
    for g in range(attended.shape[0] // requests):
        result = result + jnp.dot(
            attended[g * requests : (g + 1) * requests],
            weight_ref[g * width : (g + 1) * width, :],
            preferred_element_type=F32,
        )
    store_copies(sums_ref, result.astype(WIRE))


def last_body(arrived_ref, stream_ref, fresh_ref, out_ref, pair_ref):
    head = pair_ref.shape[3]
    for b in range(pair_ref.shape[0]):
        pair_ref[b, 0] = jnp.concatenate(
            [fresh_ref[b : b + 1, :head], fresh_ref[b : b + 1, head:]], axis=0
        ).astype(jnp.bfloat16)
    result = (stream_ref[...].astype(F32) + added_up(arrived_ref)).astype(jnp.bfloat16)
    place = lax.axis_index("y") * lax.axis_size("core") + lax.axis_index("core")
    width = out_ref.shape[1]
    result = result.astype(F32)
    own = result[:, :width]
    for k in range(1, result.shape[1] // width):
        own = jnp.where(place == k, result[:, k * width : (k + 1) * width], own)
    out_ref[...] = own.astype(jnp.bfloat16)


def shards(
    hidden,
    norm_gain,
    in_weight,
    conv_weight,
    conv_bias,
    conv_state,
    xproj_weight,
    dt_weight,
    dt_bias,
    a_log,
    skip_gain,
    ssm_state,
    out_weight,
    asker_lookup_matrix,
    o_weight,
    kv_cache,
    lengths,
    page_table,
):
    requests, model_dim = hidden.shape
    block_cols = model_dim // lax.axis_size(SEQ)
    share_cols = block_cols // lax.axis_size(CHAN)
    pages_dev, block_len, pair, _, width = kv_cache.shape
    entries = asker_lookup_matrix.shape[2]
    rows = requests * (entries // width - 2)
    in_rows = far(in_weight.transpose(0, 2, 3, 1))
    dt_rows = dt_weight.transpose(0, 2, 1)
    past = conv_state.transpose(0, 2, 1, 3)
    kv_rows = kv_cache.reshape(pages_dev * block_len * pair, width)
    conv_args = (conv_weight, conv_bias, past, xproj_weight)
    state_args = (dt_bias, a_log, skip_gain, out_weight)
    matrix = asker_lookup_matrix.reshape(block_cols, entries)

    def sums_of_proj(terms):
        own = jnp.sum(exchange(terms, PLANE).astype(F32), axis=0).astype(WIRE)
        return exchange(copied(own, LINE), LINE)

    terms, signal, gate, new_conv, own_block, own_gain = mamba_in(
        far(hidden), 0, far(norm_gain), in_rows, *[far(x) for x in conv_args], None
    )
    arrived, new_ssm = mamba_out(
        sums_of_proj(terms), signal, gate, 0, dt_rows, ssm_state, *state_args, None
    )
    stream_one, terms = local_call(
        questions_body,
        [
            (arrived, None),
            (own_block, None),
            (own_gain, None),
            (matrix, None),
        ],
        [
            ((requests, block_cols), jnp.bfloat16, None),
            ((lax.axis_size("x"), requests, entries + 128), WIRE, None),
        ],
    )
    own = jnp.sum(exchange(terms, "x").astype(F32), axis=0).astype(WIRE)
    part, fresh = local_call(
        functools.partial(attention_body, block_len=block_len, dim=model_dim),
        [
            (exchange(copied(own, "z"), "z"), None),
            (kv_rows, None),
            (lengths, "scalar"),
            (page_table, None),
        ],
        [
            ((lax.axis_size("x"), rows + 8, width), WIRE, None),
            ((requests, 2 * width), F32, None),
        ],
        [pltpu.VMEM((rows, width), F32), pltpu.VMEM((rows, kv_rows.shape[0]), F32)],
    )
    (part,) = local_call(
        merge_body,
        [(exchange(part, "x"), None)],
        [((lax.axis_size("z"), rows + 8, width), WIRE, None)],
    )
    (sums,) = local_call(
        attention_out_body,
        [(exchange(part, "z"), None), (o_weight[0], None)],
        [((lax.axis_size(CHAN), requests, block_cols), WIRE, None)],
    )
    added = jnp.sum(exchange(sums, CHAN_SUM).astype(F32), axis=0)
    stream_two = (stream_one.astype(F32) + added).astype(jnp.bfloat16)
    terms, signal, gate, new_conv = mamba_in(
        exchange(copied(stream_two, SEQ), SEQ), 1, norm_gain, in_rows, *conv_args, new_conv
    )
    arrived, new_ssm = mamba_out(
        sums_of_proj(terms), signal, gate, 1, dt_rows, ssm_state, *state_args, new_ssm
    )
    hidden_out, newest_pair = local_call(
        last_body,
        [(arrived, None), (stream_two, None), (fresh, None)],
        [
            ((requests, share_cols), jnp.bfloat16, None),
            ((requests, 1, 2, width), jnp.bfloat16, None),
        ],
    )
    return hidden_out, new_ssm, new_conv.transpose(0, 2, 1, 3), newest_pair


def solution(mesh):
    split = Mesh(mesh.devices.reshape(8, 4, 4, 2), ALL)
    placed = (
        P(),
        P(),
        P(None, None, None, ALL),
        P(None, None, ALL),
        P(None, ALL),
        P(None, None, None, ALL),
        P(None, ALL, None),
        P(None, None, ALL),
        P(None, ALL),
        P(None, None, ALL),
        P(None, ALL),
        P(None, None, None, ALL),
        P(None, ALL, None),
        P(SEQ, CHAN, None),
        P(CHAN, None, SEQ),
        P(SEQ, None, None, CHAN, None),
        P(),
        P(),
    )
    return jax.shard_map(
        shards,
        mesh=split,
        in_specs=placed,
        out_specs=(
            P(None, ALL),
            P(None, None, None, ALL),
            P(None, None, None, ALL),
            P(None, CHAN, None, None),
        ),
        check_vma=False,
    )
```

```python
import functools

import jax
import jax.numpy as jnp
from jax import lax
from jax.experimental import pallas as pl
from jax.experimental.pallas import tpu as pltpu
from jax.sharding import Mesh
from jax.sharding import PartitionSpec as P

ALL = ("z", "x", "y", "core")
SEQ = ("z", "x")
SEQ_SUM = ("x", "z")
CHAN = ("y", "core")
CHAN_SUM = ("core", "y")
PLANE = ("x", "y")
LINE = ("core", "z")
CORE_FIRST = ("core", "z", "x", "y")
WIRE = jnp.bfloat16
F32 = jnp.float32

norm_eps = 1e-06
lowest_score = -1e30


def exchange(copies, axes):
    return lax.all_to_all(copies, axes, split_axis=0, concat_axis=0, tiled=True)


def copied(x, axes):
    return jnp.broadcast_to(x, (lax.axis_size(axes), *x.shape))


def whole(shape):
    return pl.BlockSpec(shape, lambda _: (0,) * len(shape))


def layer_of(shape, layer):
    return pl.BlockSpec((1, *shape[1:]), lambda _: (layer,) + (0,) * (len(shape) - 1))


def far(x):
    return pltpu.with_memory_space_constraint(x, pltpu.HBM)


def local_call(body, inputs, outputs, scratch=(), aliases={}):
    def spec(shape, layer):
        if layer in ("far", "scalar"):
            return pl.BlockSpec(memory_space=pltpu.HBM if layer == "far" else pltpu.SMEM)
        return whole(shape) if layer is None else layer_of(shape, layer)

    return pl.pallas_call(
        body,
        grid=(1,),
        in_specs=[spec(x.shape, layer) for x, layer in inputs],
        out_specs=[spec(shape, layer) for shape, _, layer in outputs],
        out_shape=[jax.ShapeDtypeStruct(shape, dtype) for shape, dtype, _ in outputs],
        scratch_shapes=list(scratch),
        input_output_aliases=aliases,
        compiler_params=pltpu.CompilerParams(vmem_limit_bytes=12 * 1024 * 1024),
    )(*[x for x, _ in inputs])


def silu(x):
    return x * lax.logistic(x)


def added_up(ref):
    total = ref[0].astype(F32)
    for k in range(1, ref.shape[0]):
        total = total + ref[k].astype(F32)
    return total


def store_copies(ref, x):
    for k in range(ref.shape[0]):
        ref[k] = x


def against_rows(a, b):
    return lax.dot_general(a, b, (((1,), (1,)), ((), ())), preferred_element_type=F32)


def mamba_in_body(layer, *refs):
    stream_ref, gain_ref, in_ref, taps_ref, bias_ref, past_ref, xproj_ref = refs[:7]
    normed_ref, held_ref, done = refs[-3:]
    terms_ref, signal_ref, gate_ref, conv_ref = refs[7:11] if layer == 0 else refs[8:12]
    dim = normed_ref.shape[1]
    pieces = done.shape[0]
    piece = dim // pieces
    copies = [
        pltpu.make_async_copy(
            in_ref.at[layer, :, :, pl.ds(k * piece, piece)],
            held_ref.at[:, :, pl.ds(k * piece, piece)],
            done.at[k],
        )
        for k in range(pieces)
    ]
    for copy in copies:
        copy.start()
    if layer == 0:
        own_ref, own_gain_ref = refs[11:13]
        width = own_ref.shape[1]
        first = pl.multiple_of(seq_index() * width, width)
        own_ref[...] = stream_ref[:, pl.ds(first, width)]
        own_gain_ref[...] = gain_ref[1:2, pl.ds(first, width)]
    gain_row = (0, None, 2)[2 * layer]
    if len(stream_ref.shape) == 2:
        x = stream_ref[...].astype(F32)
        inv_rms = lax.rsqrt(jnp.sum(x * x, axis=1, keepdims=True) / dim + norm_eps)
        normed_ref[...] = (x * inv_rms * gain_ref[gain_row : gain_row + 1, :]).astype(jnp.bfloat16)
    else:
        blocks, _, width = stream_ref.shape
        squares = jnp.zeros(stream_ref.shape[1:], F32)
        for k in range(blocks):
            x = stream_ref[k].astype(F32)
            squares = squares + x * x
        inv_rms = lax.rsqrt(jnp.sum(squares, axis=1, keepdims=True) / dim + norm_eps)
        for k in range(blocks):
            cols = slice(k * width, (k + 1) * width)
            normed_ref[:, cols] = (
                stream_ref[k].astype(F32) * inv_rms * gain_ref[gain_row : gain_row + 1, cols]
            ).astype(jnp.bfloat16)
    inputs = jnp.zeros(signal_ref.shape, F32)
    gates = jnp.zeros(signal_ref.shape, F32)
    for k, copy in enumerate(copies):
        copy.wait()
        cols = slice(k * piece, (k + 1) * piece)
        normed = normed_ref[:, cols]
        inputs = inputs + against_rows(normed, held_ref[0, :, cols])
        gates = gates + against_rows(normed, held_ref[1, :, cols])
    inputs = inputs.astype(jnp.bfloat16)
    gates = gates.astype(jnp.bfloat16)
    taps = taps_ref[0]
    conv_sum = inputs.astype(F32) * taps[3:4]
    for k in range(3):
        conv_sum = conv_sum + past_ref[0, k].astype(F32) * taps[k : k + 1]
    signal = silu(conv_sum + bias_ref[layer : layer + 1, :]).astype(jnp.bfloat16)
    terms = jnp.dot(signal, xproj_ref[0], preferred_element_type=F32)
    store_copies(terms_ref, terms.astype(WIRE))
    signal_ref[...] = signal.astype(F32)
    gate_ref[...] = silu(gates.astype(F32))
    conv_ref[0, 0] = past_ref[0, 1]
    conv_ref[0, 1] = past_ref[0, 2]
    conv_ref[0, 2] = inputs


def mamba_in(
    stream, layer, norm_gain, in_rows, conv_weight, conv_bias, past, xproj_weight, conv_so_far
):
    requests = past.shape[2]
    channels = past.shape[3]
    inputs = [
        (stream, None),
        (norm_gain, None),
        (in_rows, "far"),
        (conv_weight, layer),
        (conv_bias, None),
        (past, layer),
        (xproj_weight, layer),
    ]
    aliases = {}
    if conv_so_far is not None:
        aliases = {len(inputs): 3}
        inputs.append((conv_so_far, "far"))
    extra = []
    if layer == 0:
        width = stream.shape[1] // lax.axis_size(SEQ)
        extra = [((requests, width), jnp.bfloat16, None), ((1, width), F32, None)]
    return local_call(
        functools.partial(mamba_in_body, layer),
        inputs,
        [
            ((lax.axis_size(PLANE), requests, xproj_weight.shape[2]), WIRE, None),
            ((requests, channels), F32, None),
            ((requests, channels), F32, None),
            (past.shape, jnp.bfloat16, layer),
            *extra,
        ],
        [
            pltpu.VMEM((requests, in_rows.shape[3]), jnp.bfloat16),
            pltpu.VMEM(in_rows.shape[1:], jnp.bfloat16),
            pltpu.SemaphoreType.DMA((4,)),
        ],
        aliases,
    )


def store_shares(shares_ref, block, x):
    row = lax.broadcasted_iota(jnp.int32, (8, 128), 0)
    group = lax.broadcasted_iota(jnp.int32, (8, 128), 1) // 32
    own = row // 2 == group
    packed = []
    for half in range(2):
        tile = x[:, half * 128 : (half + 1) * 128]
        turned = [tile] + [pltpu.roll(tile, 32 * k, 1) for k in range(1, 4)]
        for q in range(4):
            z = turned[-q % 4]
            for g in range(1, 4):
                z = jnp.where(group == g, turned[(g - q) % 4], z)
            z = jnp.where(own, z, 0.0)
            z = z + pltpu.roll(z, 4, 0)
            packed.append(z + pltpu.roll(z, 2, 0))
    for core in range(2):
        lines = packed[core]
        for k in range(1, 4):
            lines = jnp.where(row // 2 == k, packed[2 * k + core], lines)
        shares_ref[core, block * 8 : block * 8 + 8, :] = lines.astype(WIRE)


def mamba_out_body(layer, order, *refs):
    arrived_ref, signal_ref, gate_ref, dt_ref, bias_ref, decay_ref, skip_ref, state_ref, out_ref = (
        refs[:9]
    )
    blocks_ref, fresh_ref, held_ref, done = refs[-4:]
    pieces = done.shape[0]
    piece = held_ref.shape[1] // pieces
    copies = [
        pltpu.make_async_copy(
            out_ref.at[layer, :, pl.ds(k * piece, piece)],
            held_ref.at[:, pl.ds(k * piece, piece)],
            done.at[k],
        )
        for k in range(pieces)
    ]
    for copy in copies:
        copy.start()
    mapped = added_up(arrived_ref)
    low_rank = dt_ref.shape[2]
    states = decay_ref.shape[1]
    low = mapped[:, :low_rank].astype(jnp.bfloat16)
    raw = against_rows(low, dt_ref[0]) + bias_ref[layer : layer + 1, :]
    step = jnp.maximum(raw, 0.0) + jnp.log1p(jnp.exp(-jnp.abs(raw)))
    signal = signal_ref[...]
    pushed = step * signal
    rates = jnp.exp(decay_ref[0])
    rest = mapped[:, low_rank:]
    eye = lax.broadcasted_iota(jnp.int32, (states, states), 0) == lax.broadcasted_iota(
        jnp.int32, (states, states), 1
    )

    def column(row):
        return jnp.sum(jnp.where(eye, row, 0.0), axis=1, keepdims=True)

    readouts = []
    for b in range(mapped.shape[0]):
        b_in = column(rest[b : b + 1, :states])
        c_out = column(rest[b : b + 1, states : 2 * states])
        fresh = (
            jnp.exp(-step[b : b + 1] * rates) * state_ref[0, b] + pushed[b : b + 1] * b_in
        )
        fresh_ref[0, b] = fresh
        readouts.append(jnp.sum(fresh * c_out, axis=0, keepdims=True))
    readout = jnp.concatenate(readouts, axis=0) + skip_ref[layer : layer + 1, :] * signal
    gated = (readout * gate_ref[...]).astype(jnp.bfloat16)
    width = held_ref.shape[1] // len(order)
    for block in range(len(order)):
        if block * width % piece == 0:
            copies[block * width // piece].wait()
        result = jnp.dot(
            gated,
            held_ref[:, block * width : (block + 1) * width],
            preferred_element_type=F32,
        )
        if layer == 0:
            blocks_ref[order.index(block)] = result.astype(WIRE)
        else:
            store_shares(blocks_ref, block, result)


def mamba_out(
    arrived, signal, gate, layer, dt_rows, ssm_state, dt_bias, a_log, skip_gain, out_weight, so_far
):
    wide, deep = (lax.axis_size(axis) for axis in SEQ_SUM)
    order = [k * wide + j for j in range(wide) for k in range(deep)]
    inputs = [
        (arrived, None),
        (signal, None),
        (gate, None),
        (dt_rows, min(layer, dt_rows.shape[0] - 1)),
        (dt_bias, None),
        (a_log, layer),
        (skip_gain, None),
        (ssm_state, min(layer, ssm_state.shape[0] - 1)),
        (far(out_weight), "far"),
    ]
    aliases = {}
    if so_far is not None:
        aliases = {len(inputs): 1}
        inputs.append((so_far, "far"))
    blocks, fresh = local_call(
        functools.partial(mamba_out_body, layer, order),
        inputs,
        [
            (
                (wide * deep, signal.shape[0], out_weight.shape[2] // (wide * deep))
                if layer == 0
                else (2, lax.axis_size(ALL), 128),
                WIRE,
                None,
            ),
            ((a_log.shape[0], *ssm_state.shape[1:]), F32, layer),
        ],
        [pltpu.VMEM(out_weight.shape[1:], jnp.bfloat16), pltpu.SemaphoreType.DMA((4,))],
        aliases,
    )
    if layer:
        shares = exchange(blocks.reshape(-1, 2, 128), CORE_FIRST)
        return shares.reshape(-1, 128), fresh
    arrived = exchange(blocks, SEQ_SUM)
    own = jnp.sum(arrived.astype(F32), axis=0).astype(WIRE)
    return exchange(copied(own, CHAN_SUM), CHAN_SUM), fresh


def two_parts(x):
    high = x.astype(WIRE).astype(F32)
    return high, x - high


def questions_body(arrived_ref, hidden_ref, gain_ref, matrix_ref, stream_ref, terms_ref):
    stream = (hidden_ref[...].astype(F32) + added_up(arrived_ref)).astype(jnp.bfloat16)
    stream_ref[...] = stream
    wide = stream.astype(F32)
    high, low = two_parts(jnp.sum(wide * wide, axis=1, keepdims=True))
    scaled = (wide * gain_ref[...]).astype(jnp.bfloat16)
    terms = jnp.dot(scaled, matrix_ref[...], preferred_element_type=F32)
    lane = lax.broadcasted_iota(jnp.int32, (stream.shape[0], 128), 1)
    notes = jnp.where(lane == 0, high, jnp.where(lane == 1, low, 0.0))
    entries = terms.shape[1]
    for k in range(terms_ref.shape[0]):
        terms_ref[k, :, :entries] = terms.astype(WIRE)
        terms_ref[k, :, entries:] = notes.astype(WIRE)


def seq_index():
    return lax.axis_index("z") * lax.axis_size("x") + lax.axis_index("x")


def flip(x):
    n = max(x.shape)
    eye = lax.broadcasted_iota(jnp.int32, (n, n), 0) == lax.broadcasted_iota(jnp.int32, (n, n), 1)
    return jnp.sum(jnp.where(eye, x, 0.0), axis=x.shape.index(n), keepdims=True)


def store_part(out_ref, top, total, mixed):
    rows, width = mixed.shape
    high, low = two_parts(top)
    pad = jnp.zeros((1, width - rows), F32)
    notes = [jnp.concatenate([v, pad], axis=1) for v in (high, low, total)]
    notes = jnp.concatenate([*notes, jnp.zeros((out_ref.shape[1] - rows - 3, width), F32)], axis=0)
    for k in range(out_ref.shape[0]):
        out_ref[k, :rows, :] = mixed.astype(WIRE)
        out_ref[k, rows:, :] = notes.astype(WIRE)


def merged(arrived_ref):
    parts, stored, _ = arrived_ref.shape
    rows = stored - 8
    notes = [arrived_ref[k, rows:, :].astype(F32) for k in range(parts)]
    tops = [v[0:1, :rows] + v[1:2, :rows] for v in notes]
    top = tops[0]
    for v in tops[1:]:
        top = jnp.maximum(top, v)
    total = jnp.zeros_like(top)
    mixed = jnp.zeros((rows, arrived_ref.shape[2]), F32)
    for k in range(parts):
        scale = jnp.exp(tops[k] - top)
        total = total + scale * notes[k][2:3, :rows]
        mixed = mixed + flip(scale) * arrived_ref[k, :rows, :].astype(F32)
    return top, total, mixed


def attention_body(
    arrived_ref, kv_ref, lengths_ref, table_ref, part_ref, pair_ref, questions_ref, scores_ref, *, block_len, dim
):
    summed = added_up(arrived_ref)
    requests = summed.shape[0]
    width = kv_ref.shape[1]
    entries = summed.shape[1] - 128
    group_size = entries // width - 2
    rows = requests * group_size
    tokens = kv_ref.shape[0]
    chunk = 2 * block_len
    inv_rms = lax.rsqrt((summed[:, entries : entries + 1] + summed[:, entries + 1 : entries + 2]) / dim + norm_eps)
    qkv = (summed[:, :entries] * inv_rms).astype(jnp.bfloat16)
    fresh = qkv[:, group_size * width :]
    fresh = fresh.astype(F32)
    pair_ref[...] = fresh
    fresh_scores = []
    for g in range(group_size):
        one = qkv[:, g * width : (g + 1) * width]
        questions_ref[g * requests : (g + 1) * requests, :] = one.astype(F32)
        fresh_scores.append(jnp.sum(one.astype(F32) * fresh[:, :width], axis=1, keepdims=True))
    questions = questions_ref[...].astype(jnp.bfloat16)
    inv_sqrt = width ** (-0.5)
    is_first = seq_index() == 0
    fresh_score = jnp.where(is_first, jnp.concatenate(fresh_scores, axis=0) * inv_sqrt, lowest_score)
    first_slot = seq_index() * (tokens // chunk)
    table = table_ref[...]
    row = lax.broadcasted_iota(jnp.int32, table.shape, 0)
    lengths = jnp.zeros(table.shape, jnp.int32)
    for b in range(requests):
        lengths = jnp.where(row == b, lengths_ref[b], lengths)
    left = jnp.clip(
        lengths - lax.broadcasted_iota(jnp.int32, table.shape, 1) * block_len, 0, block_len
    )
    place = lax.broadcasted_iota(jnp.int32, (requests, chunk), 1)
    limit = jnp.where(place % 2 == 0, place // 2, block_len)
    top = fresh_score
    hidden_from = []
    for k in range(tokens // chunk):
        filled = jnp.sum(jnp.where(table == first_slot + k, left, 0), axis=1, keepdims=True)
        visible = jnp.concatenate([(limit < filled).astype(F32)] * group_size, axis=0) > 0.5
        hidden_from.append(visible)
        scores = against_rows(questions, kv_ref[k * chunk : (k + 1) * chunk, :]) * inv_sqrt
        scores = jnp.where(visible, scores, lowest_score)
        scores_ref[:, k * chunk : (k + 1) * chunk] = scores
        top = jnp.maximum(top, jnp.max(scores, axis=1, keepdims=True))
    high, low = two_parts(top)
    top = high + low.astype(WIRE).astype(F32)
    weight = jnp.where(is_first, jnp.exp(fresh_score - top), 0.0)
    total = weight
    values = jnp.concatenate([fresh[:, width:]] * group_size, axis=0)
    mixed = weight * values
    for k in range(tokens // chunk):
        weight = jnp.where(
            hidden_from[k], jnp.exp(scores_ref[:, k * chunk : (k + 1) * chunk] - top), 0.0
        )
        total = total + jnp.sum(weight, axis=1, keepdims=True)
        moved = pltpu.roll(weight, 1, 1).astype(jnp.bfloat16)
        mixed = mixed + jnp.dot(moved, kv_ref[k * chunk : (k + 1) * chunk, :], preferred_element_type=F32)
    store_part(part_ref, flip(top), flip(total), mixed)


def merge_body(arrived_ref, part_ref):
    top, total, mixed = merged(arrived_ref)
    store_part(part_ref, top, total, mixed)


def attention_out_body(arrived_ref, weight_ref, sums_ref):
    _, total, mixed = merged(arrived_ref)
    attended = (mixed / flip(total)).astype(jnp.bfloat16)
    requests = sums_ref.shape[1]
    width = attended.shape[1]
    result = jnp.zeros(sums_ref.shape[1:], F32)
    for g in range(attended.shape[0] // requests):
        result = result + jnp.dot(
            attended[g * requests : (g + 1) * requests],
            weight_ref[g * width : (g + 1) * width, :],
            preferred_element_type=F32,
        )
    store_copies(sums_ref, result.astype(WIRE))


def last_body(arrived_ref, stream_ref, fresh_ref, out_ref, pair_ref):
    head = pair_ref.shape[3]
    for b in range(pair_ref.shape[0]):
        pair_ref[b, 0] = jnp.concatenate(
            [fresh_ref[b : b + 1, :head], fresh_ref[b : b + 1, head:]], axis=0
        ).astype(jnp.bfloat16)
    total = jnp.zeros((8, 128), F32)
    for k in range(arrived_ref.shape[0] // 8):
        total = total + arrived_ref[k * 8 : (k + 1) * 8, :].astype(F32)
    total = total + pltpu.roll(total, 4, 0)
    total = total + pltpu.roll(total, 2, 0)
    row = lax.broadcasted_iota(jnp.int32, (8, 128), 0)
    added = total
    for k in range(1, 4):
        added = jnp.where(row // 2 == k, pltpu.roll(total, 128 - 32 * k, 1), added)
    place = lax.axis_index("y") * lax.axis_size("core") + lax.axis_index("core")
    width = out_ref.shape[1]
    stream = stream_ref[...].astype(F32)
    own = stream[:, :width]
    for k in range(1, stream.shape[1] // width):
        own = jnp.where(place == k, stream[:, k * width : (k + 1) * width], own)
    out_ref[...] = (own + added[:, :width]).astype(jnp.bfloat16)


def shards(
    hidden,
    norm_gain,
    in_weight,
    conv_weight,
    conv_bias,
    conv_state,
    xproj_weight,
    dt_weight,
    dt_bias,
    a_log,
    skip_gain,
    ssm_state,
    out_weight,
    asker_lookup_matrix,
    o_weight,
    kv_cache,
    lengths,
    page_table,
):
    requests, model_dim = hidden.shape
    block_cols = model_dim // lax.axis_size(SEQ)
    share_cols = block_cols // lax.axis_size(CHAN)
    pages_dev, block_len, pair, _, width = kv_cache.shape
    entries = asker_lookup_matrix.shape[2]
    rows = requests * (entries // width - 2)
    in_rows = far(in_weight.transpose(0, 2, 3, 1))
    dt_rows = dt_weight.transpose(0, 2, 1)
    past = conv_state.transpose(0, 2, 1, 3)
    kv_rows = kv_cache.reshape(pages_dev * block_len * pair, width)
    conv_args = (conv_weight, conv_bias, past, xproj_weight)
    state_args = (dt_bias, a_log, skip_gain, out_weight)
    matrix = asker_lookup_matrix.reshape(block_cols, entries)

    def sums_of_proj(terms):
        own = jnp.sum(exchange(terms, PLANE).astype(F32), axis=0).astype(WIRE)
        return exchange(copied(own, LINE), LINE)

    terms, signal, gate, new_conv, own_block, own_gain = mamba_in(
        far(hidden), 0, far(norm_gain), in_rows, *[far(x) for x in conv_args], None
    )
    arrived, new_ssm = mamba_out(
        sums_of_proj(terms), signal, gate, 0, dt_rows, ssm_state, *state_args, None
    )
    stream_one, terms = local_call(
        questions_body,
        [
            (arrived, None),
            (own_block, None),
            (own_gain, None),
            (matrix, None),
        ],
        [
            ((requests, block_cols), jnp.bfloat16, None),
            ((lax.axis_size("x"), requests, entries + 128), WIRE, None),
        ],
    )
    own = jnp.sum(exchange(terms, "x").astype(F32), axis=0).astype(WIRE)
    part, fresh = local_call(
        functools.partial(attention_body, block_len=block_len, dim=model_dim),
        [
            (exchange(copied(own, "z"), "z"), None),
            (kv_rows, None),
            (lengths, "scalar"),
            (page_table, None),
        ],
        [
            ((lax.axis_size("x"), rows + 8, width), WIRE, None),
            ((requests, 2 * width), F32, None),
        ],
        [pltpu.VMEM((rows, width), F32), pltpu.VMEM((rows, kv_rows.shape[0]), F32)],
    )
    (part,) = local_call(
        merge_body,
        [(exchange(part, "x"), None)],
        [((lax.axis_size("z"), rows + 8, width), WIRE, None)],
    )
    (sums,) = local_call(
        attention_out_body,
        [(exchange(part, "z"), None), (o_weight[0], None)],
        [((lax.axis_size(CHAN), requests, block_cols), WIRE, None)],
    )
    added = jnp.sum(exchange(sums, CHAN_SUM).astype(F32), axis=0)
    stream_two = (stream_one.astype(F32) + added).astype(jnp.bfloat16)
    terms, signal, gate, new_conv = mamba_in(
        exchange(copied(stream_two, SEQ), SEQ), 1, norm_gain, in_rows, *conv_args, new_conv
    )
    arrived, new_ssm = mamba_out(
        sums_of_proj(terms), signal, gate, 1, dt_rows, ssm_state, *state_args, new_ssm
    )
    hidden_out, newest_pair = local_call(
        last_body,
        [(arrived, None), (stream_two, None), (fresh, None)],
        [
            ((requests, share_cols), jnp.bfloat16, None),
            ((requests, 1, 2, width), jnp.bfloat16, None),
        ],
    )
    return hidden_out, new_ssm, new_conv.transpose(0, 2, 1, 3), newest_pair


def solution(mesh):
    split = Mesh(mesh.devices.reshape(8, 4, 4, 2), ALL)
    placed = (
        P(),
        P(),
        P(None, None, None, ALL),
        P(None, None, ALL),
        P(None, ALL),
        P(None, None, None, ALL),
        P(None, ALL, None),
        P(None, None, ALL),
        P(None, ALL),
        P(None, None, ALL),
        P(None, ALL),
        P(None, None, None, ALL),
        P(None, ALL, None),
        P(SEQ, CHAN, None),
        P(CHAN, None, SEQ),
        P(SEQ, None, None, CHAN, None),
        P(),
        P(),
    )
    return jax.shard_map(
        shards,
        mesh=split,
        in_specs=placed,
        out_specs=(
            P(None, ALL),
            P(None, None, None, ALL),
            P(None, None, None, ALL),
            P(None, CHAN, None, None),
        ),
        check_vma=False,
    )
```

```python
import functools

import jax
import jax.numpy as jnp
from jax import lax
from jax.experimental import pallas as pl
from jax.experimental.pallas import tpu as pltpu
from jax.sharding import Mesh
from jax.sharding import PartitionSpec as P

ALL = ("z", "x", "y", "core")
SEQ = ("z", "x")
SEQ_SUM = ("x", "z")
CHAN = ("y", "core")
CHAN_SUM = ("core", "y")
PLANE = ("x", "y")
LINE = ("core", "z")
CORE_FIRST = ("core", "z", "x", "y")
WIRE = jnp.bfloat16
F32 = jnp.float32

norm_eps = 1e-06
lowest_score = -1e30


def exchange(copies, axes):
    return lax.all_to_all(copies, axes, split_axis=0, concat_axis=0, tiled=True)


def copied(x, axes):
    return jnp.broadcast_to(x, (lax.axis_size(axes), *x.shape))


def whole(shape):
    return pl.BlockSpec(shape, lambda _: (0,) * len(shape))


def layer_of(shape, layer):
    return pl.BlockSpec((1, *shape[1:]), lambda _: (layer,) + (0,) * (len(shape) - 1))


def far(x):
    return pltpu.with_memory_space_constraint(x, pltpu.HBM)


def local_call(body, inputs, outputs, scratch=(), aliases={}):
    def spec(shape, layer):
        if layer in ("far", "scalar"):
            return pl.BlockSpec(memory_space=pltpu.HBM if layer == "far" else pltpu.SMEM)
        return whole(shape) if layer is None else layer_of(shape, layer)

    return pl.pallas_call(
        body,
        grid=(1,),
        in_specs=[spec(x.shape, layer) for x, layer in inputs],
        out_specs=[spec(shape, layer) for shape, _, layer in outputs],
        out_shape=[jax.ShapeDtypeStruct(shape, dtype) for shape, dtype, _ in outputs],
        scratch_shapes=list(scratch),
        input_output_aliases=aliases,
        compiler_params=pltpu.CompilerParams(vmem_limit_bytes=12 * 1024 * 1024),
    )(*[x for x, _ in inputs])


def silu(x):
    return x * lax.logistic(x)


def added_up(ref):
    total = ref[0].astype(F32)
    for k in range(1, ref.shape[0]):
        total = total + ref[k].astype(F32)
    return total


def store_copies(ref, x):
    for k in range(ref.shape[0]):
        ref[k] = x


def against_rows(a, b):
    return lax.dot_general(a, b, (((1,), (1,)), ((), ())), preferred_element_type=F32)


def mamba_in_body(layer, *refs):
    stream_ref, gain_ref, in_ref, taps_ref, bias_ref, past_ref, xproj_ref = refs[:7]
    normed_ref, held_ref, done = refs[-3:]
    terms_ref, signal_ref, gate_ref, conv_ref = refs[7:11] if layer == 0 else refs[8:12]
    dim = normed_ref.shape[1]
    pieces = done.shape[0]
    piece = dim // pieces
    copies = [
        pltpu.make_async_copy(
            in_ref.at[layer, :, :, pl.ds(k * piece, piece)],
            held_ref.at[:, :, pl.ds(k * piece, piece)],
            done.at[k],
        )
        for k in range(pieces)
    ]
    for copy in copies:
        copy.start()
    if layer == 0:
        own_ref, own_gain_ref = refs[11:13]
        width = own_ref.shape[1]
        first = pl.multiple_of(seq_index() * width, width)
        own_ref[...] = stream_ref[:, pl.ds(first, width)]
        own_gain_ref[...] = gain_ref[1:2, pl.ds(first, width)]
    gain_row = (0, None, 2)[2 * layer]
    if len(stream_ref.shape) == 2:
        x = stream_ref[...].astype(F32)
        inv_rms = lax.rsqrt(jnp.sum(x * x, axis=1, keepdims=True) / dim + norm_eps)
        normed_ref[...] = (x * inv_rms * gain_ref[gain_row : gain_row + 1, :]).astype(jnp.bfloat16)
    else:
        blocks, _, width = stream_ref.shape
        squares = jnp.zeros(stream_ref.shape[1:], F32)
        for k in range(blocks):
            x = stream_ref[k].astype(F32)
            squares = squares + x * x
        inv_rms = lax.rsqrt(jnp.sum(squares, axis=1, keepdims=True) / dim + norm_eps)
        wide, deep = (lax.axis_size(axis) for axis in SEQ_SUM)
        for k in range(blocks):
            block = k % deep * wide + k // deep
            cols = slice(block * width, (block + 1) * width)
            normed_ref[:, cols] = (
                stream_ref[k].astype(F32) * inv_rms * gain_ref[gain_row : gain_row + 1, cols]
            ).astype(jnp.bfloat16)
    inputs = jnp.zeros(signal_ref.shape, F32)
    gates = jnp.zeros(signal_ref.shape, F32)
    for k, copy in enumerate(copies):
        copy.wait()
        cols = slice(k * piece, (k + 1) * piece)
        normed = normed_ref[:, cols]
        inputs = inputs + against_rows(normed, held_ref[0, :, cols])
        gates = gates + against_rows(normed, held_ref[1, :, cols])
    inputs = inputs.astype(jnp.bfloat16)
    gates = gates.astype(jnp.bfloat16)
    taps = taps_ref[0]
    conv_sum = inputs.astype(F32) * taps[3:4]
    for k in range(3):
        conv_sum = conv_sum + past_ref[0, k].astype(F32) * taps[k : k + 1]
    signal = silu(conv_sum + bias_ref[layer : layer + 1, :]).astype(jnp.bfloat16)
    terms = jnp.dot(signal, xproj_ref[0], preferred_element_type=F32)
    store_copies(terms_ref, terms.astype(WIRE))
    signal_ref[...] = signal.astype(F32)
    gate_ref[...] = silu(gates.astype(F32))
    conv_ref[0, 0] = past_ref[0, 1]
    conv_ref[0, 1] = past_ref[0, 2]
    conv_ref[0, 2] = inputs


def mamba_in(
    stream, layer, norm_gain, in_rows, conv_weight, conv_bias, past, xproj_weight, conv_so_far
):
    requests = past.shape[2]
    channels = past.shape[3]
    inputs = [
        (stream, None),
        (norm_gain, None),
        (in_rows, "far"),
        (conv_weight, layer),
        (conv_bias, None),
        (past, layer),
        (xproj_weight, layer),
    ]
    aliases = {}
    if conv_so_far is not None:
        aliases = {len(inputs): 3}
        inputs.append((conv_so_far, "far"))
    extra = []
    if layer == 0:
        width = stream.shape[1] // lax.axis_size(SEQ)
        extra = [((requests, width), jnp.bfloat16, None), ((1, width), F32, None)]
    return local_call(
        functools.partial(mamba_in_body, layer),
        inputs,
        [
            ((lax.axis_size(PLANE), requests, xproj_weight.shape[2]), WIRE, None),
            ((requests, channels), F32, None),
            ((requests, channels), F32, None),
            (past.shape, jnp.bfloat16, layer),
            *extra,
        ],
        [
            pltpu.VMEM((requests, in_rows.shape[3]), jnp.bfloat16),
            pltpu.VMEM(in_rows.shape[1:], jnp.bfloat16),
            pltpu.SemaphoreType.DMA((4,)),
        ],
        aliases,
    )


def store_shares(shares_ref, block, x):
    row = lax.broadcasted_iota(jnp.int32, (8, 128), 0)
    group = lax.broadcasted_iota(jnp.int32, (8, 128), 1) // 32
    own = row // 2 == group
    packed = []
    for half in range(2):
        tile = x[:, half * 128 : (half + 1) * 128]
        turned = [tile] + [pltpu.roll(tile, 32 * k, 1) for k in range(1, 4)]
        for q in range(4):
            z = turned[-q % 4]
            for g in range(1, 4):
                z = jnp.where(group == g, turned[(g - q) % 4], z)
            z = jnp.where(own, z, 0.0)
            z = z + pltpu.roll(z, 4, 0)
            packed.append(z + pltpu.roll(z, 2, 0))
    for core in range(2):
        lines = packed[core]
        for k in range(1, 4):
            lines = jnp.where(row // 2 == k, packed[2 * k + core], lines)
        shares_ref[core, block * 8 : block * 8 + 8, :] = lines.astype(WIRE)


def mamba_out_body(layer, order, *refs):
    arrived_ref, signal_ref, gate_ref, dt_ref, bias_ref, decay_ref, skip_ref, state_ref, out_ref = (
        refs[:9]
    )
    blocks_ref, fresh_ref = refs[9:11] if layer == 0 else refs[10:12]
    if layer == 0:
        held_ref, done = refs[11:]
    else:
        held_ref = out_ref.at[0]
    pieces = 2 if layer == 0 else 0
    piece = out_ref.shape[2] // max(pieces, 1)
    copies = [
        pltpu.make_async_copy(
            out_ref.at[layer, :, pl.ds(k * piece, piece)],
            held_ref.at[:, pl.ds(k * piece, piece)],
            done.at[k],
        )
        for k in range(pieces)
    ]
    for copy in copies:
        copy.start()
    mapped = added_up(arrived_ref)
    low_rank = dt_ref.shape[2]
    states = decay_ref.shape[1]
    low = mapped[:, :low_rank].astype(jnp.bfloat16)
    raw = against_rows(low, dt_ref[0]) + bias_ref[layer : layer + 1, :]
    step = jnp.maximum(raw, 0.0) + jnp.log1p(jnp.exp(-jnp.abs(raw)))
    signal = signal_ref[...]
    pushed = step * signal
    rates = jnp.exp(decay_ref[0])
    rest = mapped[:, low_rank:]
    eye = lax.broadcasted_iota(jnp.int32, (states, states), 0) == lax.broadcasted_iota(
        jnp.int32, (states, states), 1
    )

    def column(row):
        return jnp.sum(jnp.where(eye, row, 0.0), axis=1, keepdims=True)

    readouts = []
    for b in range(mapped.shape[0]):
        b_in = column(rest[b : b + 1, :states])
        c_out = column(rest[b : b + 1, states : 2 * states])
        fresh = (
            jnp.exp(-step[b : b + 1] * rates) * state_ref[0, b] + pushed[b : b + 1] * b_in
        )
        fresh_ref[0, b] = fresh
        readouts.append(jnp.sum(fresh * c_out, axis=0, keepdims=True))
    readout = jnp.concatenate(readouts, axis=0) + skip_ref[layer : layer + 1, :] * signal
    gated = (readout * gate_ref[...]).astype(jnp.bfloat16)
    width = out_ref.shape[2] // len(order)
    for block in range(len(order)):
        if layer == 0 and block * width % piece == 0:
            copies[block * width // piece].wait()
        result = jnp.dot(
            gated,
            held_ref[:, block * width : (block + 1) * width],
            preferred_element_type=F32,
        )
        if layer == 0:
            blocks_ref[order.index(block)] = result.astype(WIRE)
        else:
            store_shares(blocks_ref, block, result)


def mamba_out(
    arrived, signal, gate, layer, dt_rows, ssm_state, dt_bias, a_log, skip_gain, out_weight, so_far
):
    wide, deep = (lax.axis_size(axis) for axis in SEQ_SUM)
    order = [k * wide + j for j in range(wide) for k in range(deep)]
    inputs = [
        (arrived, None),
        (signal, None),
        (gate, None),
        (dt_rows, min(layer, dt_rows.shape[0] - 1)),
        (dt_bias, None),
        (a_log, layer),
        (skip_gain, None),
        (ssm_state, min(layer, ssm_state.shape[0] - 1)),
        (far(out_weight), "far") if layer == 0 else (out_weight, layer),
    ]
    aliases = {}
    if so_far is not None:
        aliases = {len(inputs): 1}
        inputs.append((so_far, "far"))
    blocks, fresh = local_call(
        functools.partial(mamba_out_body, layer, order),
        inputs,
        [
            (
                (wide * deep, signal.shape[0], out_weight.shape[2] // (wide * deep))
                if layer == 0
                else (2, lax.axis_size(ALL), 128),
                WIRE,
                None,
            ),
            ((a_log.shape[0], *ssm_state.shape[1:]), F32, layer),
        ],
        [pltpu.VMEM(out_weight.shape[1:], jnp.bfloat16), pltpu.SemaphoreType.DMA((2,))]
        if layer == 0
        else [],
        aliases,
    )
    if layer:
        shares = exchange(blocks.reshape(-1, 2, 128), CORE_FIRST)
        return shares.reshape(-1, 128), fresh
    arrived = exchange(blocks, SEQ_SUM)
    own = jnp.sum(arrived.astype(F32), axis=0).astype(WIRE)
    return exchange(copied(own, CHAN_SUM), CHAN_SUM), fresh


def two_parts(x):
    high = x.astype(WIRE).astype(F32)
    return high, x - high


def questions_body(arrived_ref, hidden_ref, gain_ref, matrix_ref, stream_ref, terms_ref):
    stream = (hidden_ref[...].astype(F32) + added_up(arrived_ref)).astype(jnp.bfloat16)
    stream_ref[...] = stream
    wide = stream.astype(F32)
    high, low = two_parts(jnp.sum(wide * wide, axis=1, keepdims=True))
    scaled = (wide * gain_ref[...]).astype(jnp.bfloat16)
    terms = jnp.dot(scaled, matrix_ref[...], preferred_element_type=F32)
    lane = lax.broadcasted_iota(jnp.int32, (stream.shape[0], 128), 1)
    notes = jnp.where(lane == 0, high, jnp.where(lane == 1, low, 0.0))
    entries = terms.shape[1]
    for k in range(terms_ref.shape[0]):
        terms_ref[k, :, :entries] = terms.astype(WIRE)
        terms_ref[k, :, entries:] = notes.astype(WIRE)


def seq_index():
    return lax.axis_index("z") * lax.axis_size("x") + lax.axis_index("x")


def flip(x):
    n = max(x.shape)
    eye = lax.broadcasted_iota(jnp.int32, (n, n), 0) == lax.broadcasted_iota(jnp.int32, (n, n), 1)
    return jnp.sum(jnp.where(eye, x, 0.0), axis=x.shape.index(n), keepdims=True)


def store_part(out_ref, top, total, mixed):
    rows, width = mixed.shape
    high, low = two_parts(top)
    pad = jnp.zeros((1, width - rows), F32)
    notes = [jnp.concatenate([v, pad], axis=1) for v in (high, low, total)]
    notes = jnp.concatenate([*notes, jnp.zeros((out_ref.shape[1] - rows - 3, width), F32)], axis=0)
    for k in range(out_ref.shape[0]):
        out_ref[k, :rows, :] = mixed.astype(WIRE)
        out_ref[k, rows:, :] = notes.astype(WIRE)


def merged(arrived_ref):
    parts, stored, _ = arrived_ref.shape
    rows = stored - 8
    notes = [arrived_ref[k, rows:, :].astype(F32) for k in range(parts)]
    tops = [v[0:1, :rows] + v[1:2, :rows] for v in notes]
    top = tops[0]
    for v in tops[1:]:
        top = jnp.maximum(top, v)
    total = jnp.zeros_like(top)
    mixed = jnp.zeros((rows, arrived_ref.shape[2]), F32)
    for k in range(parts):
        scale = jnp.exp(tops[k] - top)
        total = total + scale * notes[k][2:3, :rows]
        mixed = mixed + flip(scale) * arrived_ref[k, :rows, :].astype(F32)
    return top, total, mixed


def attention_body(
    arrived_ref,
    cache_ref,
    lengths_ref,
    table_ref,
    part_ref,
    pair_ref,
    questions_ref,
    scores_ref,
    kv_ref,
    done,
    *,
    block_len,
    dim,
):
    copies = []
    for k in range(done.shape[0]):
        slot_rows = pl.ds(k * 2 * block_len, 2 * block_len)
        copies.append(
            pltpu.make_async_copy(cache_ref.at[slot_rows, :], kv_ref.at[slot_rows, :], done.at[k])
        )
        copies[-1].start()
    summed = added_up(arrived_ref)
    requests = summed.shape[0]
    width = kv_ref.shape[1]
    entries = summed.shape[1] - 128
    group_size = entries // width - 2
    rows = requests * group_size
    tokens = kv_ref.shape[0]
    chunk = 2 * block_len
    inv_rms = lax.rsqrt((summed[:, entries : entries + 1] + summed[:, entries + 1 : entries + 2]) / dim + norm_eps)
    qkv = (summed[:, :entries] * inv_rms).astype(jnp.bfloat16)
    fresh = qkv[:, group_size * width :]
    fresh = fresh.astype(F32)
    pair_ref[...] = fresh
    fresh_scores = []
    for g in range(group_size):
        one = qkv[:, g * width : (g + 1) * width]
        questions_ref[g * requests : (g + 1) * requests, :] = one.astype(F32)
        fresh_scores.append(jnp.sum(one.astype(F32) * fresh[:, :width], axis=1, keepdims=True))
    questions = questions_ref[...].astype(jnp.bfloat16)
    inv_sqrt = width ** (-0.5)
    is_first = seq_index() == 0
    fresh_score = jnp.where(is_first, jnp.concatenate(fresh_scores, axis=0) * inv_sqrt, lowest_score)
    first_slot = seq_index() * (tokens // chunk)
    table = table_ref[...]
    row = lax.broadcasted_iota(jnp.int32, table.shape, 0)
    lengths = jnp.zeros(table.shape, jnp.int32)
    for b in range(requests):
        lengths = jnp.where(row == b, lengths_ref[b], lengths)
    left = jnp.clip(
        lengths - lax.broadcasted_iota(jnp.int32, table.shape, 1) * block_len, 0, block_len
    )
    place = lax.broadcasted_iota(jnp.int32, (requests, chunk), 1)
    limit = jnp.where(place % 2 == 0, place // 2, block_len)
    top = fresh_score
    hidden_from = []
    for k in range(tokens // chunk):
        filled = jnp.sum(jnp.where(table == first_slot + k, left, 0), axis=1, keepdims=True)
        visible = jnp.concatenate([(limit < filled).astype(F32)] * group_size, axis=0) > 0.5
        hidden_from.append(visible)
        copies[k].wait()
        scores = against_rows(questions, kv_ref[k * chunk : (k + 1) * chunk, :]) * inv_sqrt
        scores = jnp.where(visible, scores, lowest_score)
        scores_ref[:, k * chunk : (k + 1) * chunk] = scores
        top = jnp.maximum(top, jnp.max(scores, axis=1, keepdims=True))
    high, low = two_parts(top)
    top = high + low.astype(WIRE).astype(F32)
    weight = jnp.where(is_first, jnp.exp(fresh_score - top), 0.0)
    total = weight
    values = jnp.concatenate([fresh[:, width:]] * group_size, axis=0)
    mixed = weight * values
    for k in range(tokens // chunk):
        weight = jnp.where(
            hidden_from[k], jnp.exp(scores_ref[:, k * chunk : (k + 1) * chunk] - top), 0.0
        )
        total = total + jnp.sum(weight, axis=1, keepdims=True)
        moved = pltpu.roll(weight, 1, 1).astype(jnp.bfloat16)
        mixed = mixed + jnp.dot(moved, kv_ref[k * chunk : (k + 1) * chunk, :], preferred_element_type=F32)
    store_part(part_ref, flip(top), flip(total), mixed)


def merge_body(arrived_ref, part_ref):
    top, total, mixed = merged(arrived_ref)
    store_part(part_ref, top, total, mixed)


def attention_out_body(arrived_ref, weight_ref, sums_ref):
    _, total, mixed = merged(arrived_ref)
    attended = (mixed / flip(total)).astype(jnp.bfloat16)
    requests = sums_ref.shape[1]
    width = attended.shape[1]
    result = jnp.zeros(sums_ref.shape[1:], F32)
    for g in range(attended.shape[0] // requests):
        result = result + jnp.dot(
            attended[g * requests : (g + 1) * requests],
            weight_ref[g * width : (g + 1) * width, :],
            preferred_element_type=F32,
        )
    store_copies(sums_ref, result.astype(WIRE))


def last_body(arrived_ref, stream_ref, fresh_ref, out_ref, pair_ref):
    head = pair_ref.shape[3]
    for b in range(pair_ref.shape[0]):
        pair_ref[b, 0] = jnp.concatenate(
            [fresh_ref[b : b + 1, :head], fresh_ref[b : b + 1, head:]], axis=0
        ).astype(jnp.bfloat16)
    total = jnp.zeros((8, 128), F32)
    for k in range(arrived_ref.shape[0] // 8):
        total = total + arrived_ref[k * 8 : (k + 1) * 8, :].astype(F32)
    total = total + pltpu.roll(total, 4, 0)
    total = total + pltpu.roll(total, 2, 0)
    row = lax.broadcasted_iota(jnp.int32, (8, 128), 0)
    added = total
    for k in range(1, 4):
        added = jnp.where(row // 2 == k, pltpu.roll(total, 128 - 32 * k, 1), added)
    place = lax.axis_index("y") * lax.axis_size("core") + lax.axis_index("core")
    width = out_ref.shape[1]
    stream = stream_ref[...].astype(F32)
    own = stream[:, :width]
    for k in range(1, stream.shape[1] // width):
        own = jnp.where(place == k, stream[:, k * width : (k + 1) * width], own)
    out_ref[...] = (own + added[:, :width]).astype(jnp.bfloat16)


def shards(
    hidden,
    norm_gain,
    in_weight,
    conv_weight,
    conv_bias,
    conv_state,
    xproj_weight,
    dt_weight,
    dt_bias,
    a_log,
    skip_gain,
    ssm_state,
    out_weight,
    asker_lookup_matrix,
    o_weight,
    kv_cache,
    lengths,
    page_table,
):
    requests, model_dim = hidden.shape
    block_cols = model_dim // lax.axis_size(SEQ)
    share_cols = block_cols // lax.axis_size(CHAN)
    pages_dev, block_len, pair, _, width = kv_cache.shape
    entries = asker_lookup_matrix.shape[2]
    rows = requests * (entries // width - 2)
    in_rows = far(in_weight.transpose(0, 2, 3, 1))
    dt_rows = dt_weight.transpose(0, 2, 1)
    past = conv_state.transpose(0, 2, 1, 3)
    kv_rows = kv_cache.reshape(pages_dev * block_len * pair, width)
    conv_args = (conv_weight, conv_bias, past, xproj_weight)
    state_args = (dt_bias, a_log, skip_gain, out_weight)
    matrix = asker_lookup_matrix.reshape(block_cols, entries)

    def sums_of_proj(terms):
        own = jnp.sum(exchange(terms, PLANE).astype(F32), axis=0).astype(WIRE)
        return exchange(copied(own, LINE), LINE)

    terms, signal, gate, new_conv, own_block, own_gain = mamba_in(
        far(hidden), 0, far(norm_gain), in_rows, *[far(x) for x in conv_args], None
    )
    arrived, new_ssm = mamba_out(
        sums_of_proj(terms), signal, gate, 0, dt_rows, ssm_state, *state_args, None
    )
    stream_one, terms = local_call(
        questions_body,
        [
            (arrived, None),
            (own_block, None),
            (own_gain, None),
            (matrix, None),
        ],
        [
            ((requests, block_cols), jnp.bfloat16, None),
            ((lax.axis_size("x"), requests, entries + 128), WIRE, None),
        ],
    )
    own = jnp.sum(exchange(terms, "x").astype(F32), axis=0).astype(WIRE)
    part, fresh = local_call(
        functools.partial(attention_body, block_len=block_len, dim=model_dim),
        [
            (exchange(copied(own, "z"), "z"), None),
            (far(kv_rows), "far"),
            (lengths, "scalar"),
            (page_table, None),
        ],
        [
            ((lax.axis_size("x"), rows + 8, width), WIRE, None),
            ((requests, 2 * width), F32, None),
        ],
        [
            pltpu.VMEM((rows, width), F32),
            pltpu.VMEM((rows, kv_rows.shape[0]), F32),
            pltpu.VMEM(kv_rows.shape, jnp.bfloat16),
            pltpu.SemaphoreType.DMA((pages_dev,)),
        ],
    )
    (part,) = local_call(
        merge_body,
        [(exchange(part, "x"), None)],
        [((lax.axis_size("z"), rows + 8, width), WIRE, None)],
    )
    (sums,) = local_call(
        attention_out_body,
        [(exchange(part, "z"), None), (o_weight[0], None)],
        [((lax.axis_size(CHAN), requests, block_cols), WIRE, None)],
    )
    added = jnp.sum(exchange(sums, CHAN_SUM).astype(F32), axis=0)
    stream_two = (stream_one.astype(F32) + added).astype(jnp.bfloat16)
    terms, signal, gate, new_conv = mamba_in(
        exchange(copied(stream_two, SEQ_SUM), SEQ_SUM), 1, norm_gain, in_rows, *conv_args, new_conv
    )
    arrived, new_ssm = mamba_out(
        sums_of_proj(terms), signal, gate, 1, dt_rows, ssm_state, *state_args, new_ssm
    )
    hidden_out, newest_pair = local_call(
        last_body,
        [(arrived, None), (stream_two, None), (fresh, None)],
        [
            ((requests, share_cols), jnp.bfloat16, None),
            ((requests, 1, 2, width), jnp.bfloat16, None),
        ],
    )
    return hidden_out, new_ssm, new_conv.transpose(0, 2, 1, 3), newest_pair


def solution(mesh):
    split = Mesh(mesh.devices.reshape(8, 4, 4, 2), ALL)
    placed = (
        P(),
        P(),
        P(None, None, None, ALL),
        P(None, None, ALL),
        P(None, ALL),
        P(None, None, None, ALL),
        P(None, ALL, None),
        P(None, None, ALL),
        P(None, ALL),
        P(None, None, ALL),
        P(None, ALL),
        P(None, None, None, ALL),
        P(None, ALL, None),
        P(SEQ, CHAN, None),
        P(CHAN, None, SEQ),
        P(SEQ, None, None, CHAN, None),
        P(),
        P(),
    )
    return jax.shard_map(
        shards,
        mesh=split,
        in_specs=placed,
        out_specs=(
            P(None, ALL),
            P(None, None, None, ALL),
            P(None, None, None, ALL),
            P(None, CHAN, None, None),
        ),
        check_vma=False,
    )
```

```python
import functools

import jax
import jax.numpy as jnp
from jax import lax
from jax.experimental import pallas as pl
from jax.experimental.pallas import tpu as pltpu
from jax.sharding import Mesh
from jax.sharding import PartitionSpec as P

ALL = ("z", "x", "y", "core")
SEQ = ("z", "x")
SEQ_SUM = ("x", "z")
CHAN = ("y", "core")
CHAN_SUM = ("core", "y")
PLANE = ("x", "y")
LINE = ("core", "z")
CORE_FIRST = ("core", "z", "x", "y")
WIRE = jnp.bfloat16
F32 = jnp.float32

norm_eps = 1e-06
lowest_score = -1e30


def exchange(copies, axes):
    return lax.all_to_all(copies, axes, split_axis=0, concat_axis=0, tiled=True)


def copied(x, axes):
    return jnp.broadcast_to(x, (lax.axis_size(axes), *x.shape))


def whole(shape):
    return pl.BlockSpec(shape, lambda _: (0,) * len(shape))


def layer_of(shape, layer):
    return pl.BlockSpec((1, *shape[1:]), lambda _: (layer,) + (0,) * (len(shape) - 1))


def far(x):
    return pltpu.with_memory_space_constraint(x, pltpu.HBM)


def local_call(body, inputs, outputs, scratch=(), aliases={}):
    def spec(shape, layer):
        if layer in ("far", "scalar"):
            return pl.BlockSpec(memory_space=pltpu.HBM if layer == "far" else pltpu.SMEM)
        return whole(shape) if layer is None else layer_of(shape, layer)

    return pl.pallas_call(
        body,
        grid=(1,),
        in_specs=[spec(x.shape, layer) for x, layer in inputs],
        out_specs=[spec(shape, layer) for shape, _, layer in outputs],
        out_shape=[jax.ShapeDtypeStruct(shape, dtype) for shape, dtype, _ in outputs],
        scratch_shapes=list(scratch),
        input_output_aliases=aliases,
        compiler_params=pltpu.CompilerParams(vmem_limit_bytes=12 * 1024 * 1024),
    )(*[x for x, _ in inputs])


def silu(x):
    return x * lax.logistic(x)


def added_up(ref):
    total = ref[0].astype(F32)
    for k in range(1, ref.shape[0]):
        total = total + ref[k].astype(F32)
    return total


def store_copies(ref, x):
    for k in range(ref.shape[0]):
        ref[k] = x


def against_rows(a, b):
    return lax.dot_general(a, b, (((1,), (1,)), ((), ())), preferred_element_type=F32)


def mamba_in_body(layer, *refs):
    stream_ref, gain_ref, in_ref, taps_ref, bias_ref, past_ref, xproj_ref = refs[:7]
    normed_ref, held_ref, done = refs[-3:]
    terms_ref, signal_ref, gate_ref, conv_ref = refs[7:11] if layer == 0 else refs[8:12]
    dim = normed_ref.shape[1]
    pieces = done.shape[0]
    piece = dim // pieces
    copies = [
        pltpu.make_async_copy(
            in_ref.at[layer, :, :, pl.ds(k * piece, piece)],
            held_ref.at[:, :, pl.ds(k * piece, piece)],
            done.at[k],
        )
        for k in range(pieces)
    ]
    for copy in copies:
        copy.start()
    if layer == 0:
        own_ref, own_gain_ref = refs[11:13]
        width = own_ref.shape[1]
        first = pl.multiple_of(seq_index() * width, width)
        own_ref[...] = stream_ref[:, pl.ds(first, width)]
        own_gain_ref[...] = gain_ref[1:2, pl.ds(first, width)]
    gain_row = (0, None, 2)[2 * layer]
    if len(stream_ref.shape) == 2:
        x = stream_ref[...].astype(F32)
        inv_rms = lax.rsqrt(jnp.sum(x * x, axis=1, keepdims=True) / dim + norm_eps)
        normed_ref[...] = (x * inv_rms * gain_ref[gain_row : gain_row + 1, :]).astype(jnp.bfloat16)
    else:
        blocks, _, width = stream_ref.shape
        squares = jnp.zeros(stream_ref.shape[1:], F32)
        for k in range(blocks):
            x = stream_ref[k].astype(F32)
            squares = squares + x * x
        inv_rms = lax.rsqrt(jnp.sum(squares, axis=1, keepdims=True) / dim + norm_eps)
        for k in range(blocks):
            cols = slice(k * width, (k + 1) * width)
            normed_ref[:, cols] = (
                stream_ref[k].astype(F32) * inv_rms * gain_ref[gain_row : gain_row + 1, cols]
            ).astype(jnp.bfloat16)
    inputs = jnp.zeros(signal_ref.shape, F32)
    gates = jnp.zeros(signal_ref.shape, F32)
    for k, copy in enumerate(copies):
        copy.wait()
        cols = slice(k * piece, (k + 1) * piece)
        normed = normed_ref[:, cols]
        inputs = inputs + against_rows(normed, held_ref[0, :, cols])
        gates = gates + against_rows(normed, held_ref[1, :, cols])
    inputs = inputs.astype(jnp.bfloat16)
    gates = gates.astype(jnp.bfloat16)
    taps = taps_ref[0]
    conv_sum = inputs.astype(F32) * taps[3:4]
    for k in range(3):
        conv_sum = conv_sum + past_ref[0, k].astype(F32) * taps[k : k + 1]
    signal = silu(conv_sum + bias_ref[layer : layer + 1, :]).astype(jnp.bfloat16)
    terms = jnp.dot(signal, xproj_ref[0], preferred_element_type=F32)
    store_copies(terms_ref, terms.astype(WIRE))
    signal_ref[...] = signal.astype(F32)
    gate_ref[...] = silu(gates.astype(F32))
    conv_ref[0, 0] = past_ref[0, 1]
    conv_ref[0, 1] = past_ref[0, 2]
    conv_ref[0, 2] = inputs


def mamba_in(
    stream, layer, norm_gain, in_rows, conv_weight, conv_bias, past, xproj_weight, conv_so_far
):
    requests = past.shape[2]
    channels = past.shape[3]
    inputs = [
        (stream, None),
        (norm_gain, None),
        (in_rows, "far"),
        (conv_weight, layer),
        (conv_bias, None),
        (past, layer),
        (xproj_weight, layer),
    ]
    aliases = {}
    if conv_so_far is not None:
        aliases = {len(inputs): 3}
        inputs.append((conv_so_far, "far"))
    extra = []
    if layer == 0:
        width = stream.shape[1] // lax.axis_size(SEQ)
        extra = [((requests, width), jnp.bfloat16, None), ((1, width), F32, None)]
    return local_call(
        functools.partial(mamba_in_body, layer),
        inputs,
        [
            ((lax.axis_size(PLANE), requests, xproj_weight.shape[2]), WIRE, None),
            ((requests, channels), F32, None),
            ((requests, channels), F32, None),
            (past.shape, jnp.bfloat16, layer),
            *extra,
        ],
        [
            pltpu.VMEM((requests, in_rows.shape[3]), jnp.bfloat16),
            pltpu.VMEM(in_rows.shape[1:], jnp.bfloat16),
            pltpu.SemaphoreType.DMA((4,)),
        ],
        aliases,
    )


def store_shares(shares_ref, block, x):
    row = lax.broadcasted_iota(jnp.int32, (8, 128), 0)
    group = lax.broadcasted_iota(jnp.int32, (8, 128), 1) // 32
    own = row // 2 == group
    packed = []
    for half in range(2):
        tile = x[:, half * 128 : (half + 1) * 128]
        turned = [tile] + [pltpu.roll(tile, 32 * k, 1) for k in range(1, 4)]
        for q in range(4):
            z = turned[-q % 4]
            for g in range(1, 4):
                z = jnp.where(group == g, turned[(g - q) % 4], z)
            z = jnp.where(own, z, 0.0)
            z = z + pltpu.roll(z, 4, 0)
            packed.append(z + pltpu.roll(z, 2, 0))
    for core in range(2):
        lines = packed[core]
        for k in range(1, 4):
            lines = jnp.where(row // 2 == k, packed[2 * k + core], lines)
        shares_ref[core, block * 8 : block * 8 + 8, :] = lines.astype(WIRE)


def mamba_out_body(layer, order, *refs):
    arrived_ref, signal_ref, gate_ref, dt_ref, bias_ref, decay_ref, skip_ref, state_ref, out_ref = (
        refs[:9]
    )
    blocks_ref, fresh_ref = refs[9:11] if layer == 0 else refs[10:12]
    if layer == 0:
        held_ref, done = refs[11:]
    else:
        held_ref = out_ref.at[0]
    pieces = 2 if layer == 0 else 0
    piece = out_ref.shape[2] // max(pieces, 1)
    copies = [
        pltpu.make_async_copy(
            out_ref.at[layer, :, pl.ds(k * piece, piece)],
            held_ref.at[:, pl.ds(k * piece, piece)],
            done.at[k],
        )
        for k in range(pieces)
    ]
    for copy in copies:
        copy.start()
    mapped = added_up(arrived_ref)
    low_rank = dt_ref.shape[2]
    states = decay_ref.shape[1]
    low = mapped[:, :low_rank].astype(jnp.bfloat16)
    raw = against_rows(low, dt_ref[0]) + bias_ref[layer : layer + 1, :]
    step = jnp.maximum(raw, 0.0) + jnp.log1p(jnp.exp(-jnp.abs(raw)))
    signal = signal_ref[...]
    pushed = step * signal
    rates = jnp.exp(decay_ref[0])
    rest = mapped[:, low_rank:]
    eye = lax.broadcasted_iota(jnp.int32, (states, states), 0) == lax.broadcasted_iota(
        jnp.int32, (states, states), 1
    )

    def column(row):
        return jnp.sum(jnp.where(eye, row, 0.0), axis=1, keepdims=True)

    readouts = []
    for b in range(mapped.shape[0]):
        b_in = column(rest[b : b + 1, :states])
        c_out = column(rest[b : b + 1, states : 2 * states])
        fresh = (
            jnp.exp(-step[b : b + 1] * rates) * state_ref[0, b] + pushed[b : b + 1] * b_in
        )
        fresh_ref[0, b] = fresh
        readouts.append(jnp.sum(fresh * c_out, axis=0, keepdims=True))
    readout = jnp.concatenate(readouts, axis=0) + skip_ref[layer : layer + 1, :] * signal
    gated = (readout * gate_ref[...]).astype(jnp.bfloat16)
    width = out_ref.shape[2] // len(order)
    for block in range(len(order)):
        if layer == 0 and block * width % piece == 0:
            copies[block * width // piece].wait()
        result = jnp.dot(
            gated,
            held_ref[:, block * width : (block + 1) * width],
            preferred_element_type=F32,
        )
        if layer == 0:
            blocks_ref[order.index(block)] = result.astype(WIRE)
        else:
            store_shares(blocks_ref, block, result)


def mamba_out(
    arrived, signal, gate, layer, dt_rows, ssm_state, dt_bias, a_log, skip_gain, out_weight, so_far
):
    wide, deep = (lax.axis_size(axis) for axis in SEQ_SUM)
    order = [k * wide + j for j in range(wide) for k in range(deep)]
    inputs = [
        (arrived, None),
        (signal, None),
        (gate, None),
        (dt_rows, min(layer, dt_rows.shape[0] - 1)),
        (dt_bias, None),
        (a_log, layer),
        (skip_gain, None),
        (ssm_state, min(layer, ssm_state.shape[0] - 1)),
        (far(out_weight), "far") if layer == 0 else (out_weight, layer),
    ]
    aliases = {}
    if so_far is not None:
        aliases = {len(inputs): 1}
        inputs.append((so_far, "far"))
    blocks, fresh = local_call(
        functools.partial(mamba_out_body, layer, order),
        inputs,
        [
            (
                (wide * deep, signal.shape[0], out_weight.shape[2] // (wide * deep))
                if layer == 0
                else (2, lax.axis_size(ALL), 128),
                WIRE,
                None,
            ),
            ((a_log.shape[0], *ssm_state.shape[1:]), F32, layer),
        ],
        [pltpu.VMEM(out_weight.shape[1:], jnp.bfloat16), pltpu.SemaphoreType.DMA((2,))]
        if layer == 0
        else [],
        aliases,
    )
    if layer:
        shares = exchange(blocks.reshape(-1, 2, 128), CORE_FIRST)
        return shares.reshape(-1, 128), fresh
    arrived = exchange(blocks, SEQ_SUM)
    own = jnp.sum(arrived.astype(F32), axis=0).astype(WIRE)
    return exchange(copied(own, CHAN_SUM), CHAN_SUM), fresh


def two_parts(x):
    high = x.astype(WIRE).astype(F32)
    return high, x - high


def questions_body(arrived_ref, hidden_ref, gain_ref, matrix_ref, stream_ref, terms_ref):
    stream = (hidden_ref[...].astype(F32) + added_up(arrived_ref)).astype(jnp.bfloat16)
    stream_ref[...] = stream
    wide = stream.astype(F32)
    high, low = two_parts(jnp.sum(wide * wide, axis=1, keepdims=True))
    scaled = (wide * gain_ref[...]).astype(jnp.bfloat16)
    terms = jnp.dot(scaled, matrix_ref[...], preferred_element_type=F32)
    lane = lax.broadcasted_iota(jnp.int32, (stream.shape[0], 128), 1)
    notes = jnp.where(lane == 0, high, jnp.where(lane == 1, low, 0.0))
    entries = terms.shape[1]
    for k in range(terms_ref.shape[0]):
        terms_ref[k, :, :entries] = terms.astype(WIRE)
        terms_ref[k, :, entries:] = notes.astype(WIRE)


def seq_index():
    return lax.axis_index("z") * lax.axis_size("x") + lax.axis_index("x")


def flip(x):
    n = max(x.shape)
    eye = lax.broadcasted_iota(jnp.int32, (n, n), 0) == lax.broadcasted_iota(jnp.int32, (n, n), 1)
    return jnp.sum(jnp.where(eye, x, 0.0), axis=x.shape.index(n), keepdims=True)


def store_part(out_ref, top, total, mixed):
    rows, width = mixed.shape
    high, low = two_parts(top)
    pad = jnp.zeros((1, width - rows), F32)
    notes = [jnp.concatenate([v, pad], axis=1) for v in (high, low, total)]
    notes = jnp.concatenate([*notes, jnp.zeros((out_ref.shape[1] - rows - 3, width), F32)], axis=0)
    for k in range(out_ref.shape[0]):
        out_ref[k, :rows, :] = mixed.astype(WIRE)
        out_ref[k, rows:, :] = notes.astype(WIRE)


def merged(arrived_ref):
    parts, stored, _ = arrived_ref.shape
    rows = stored - 8
    notes = [arrived_ref[k, rows:, :].astype(F32) for k in range(parts)]
    tops = [v[0:1, :rows] + v[1:2, :rows] for v in notes]
    top = tops[0]
    for v in tops[1:]:
        top = jnp.maximum(top, v)
    total = jnp.zeros_like(top)
    mixed = jnp.zeros((rows, arrived_ref.shape[2]), F32)
    for k in range(parts):
        scale = jnp.exp(tops[k] - top)
        total = total + scale * notes[k][2:3, :rows]
        mixed = mixed + flip(scale) * arrived_ref[k, :rows, :].astype(F32)
    return top, total, mixed


def attention_body(
    arrived_ref, kv_ref, lengths_ref, table_ref, part_ref, pair_ref, questions_ref, scores_ref, *, block_len, dim
):
    summed = added_up(arrived_ref)
    requests = summed.shape[0]
    width = kv_ref.shape[1]
    entries = summed.shape[1] - 128
    group_size = entries // width - 2
    rows = requests * group_size
    tokens = kv_ref.shape[0]
    chunk = 2 * block_len
    inv_rms = lax.rsqrt((summed[:, entries : entries + 1] + summed[:, entries + 1 : entries + 2]) / dim + norm_eps)
    qkv = (summed[:, :entries] * inv_rms).astype(jnp.bfloat16)
    fresh = qkv[:, group_size * width :]
    fresh = fresh.astype(F32)
    pair_ref[...] = fresh
    fresh_scores = []
    for g in range(group_size):
        one = qkv[:, g * width : (g + 1) * width]
        questions_ref[g * requests : (g + 1) * requests, :] = one.astype(F32)
        fresh_scores.append(jnp.sum(one.astype(F32) * fresh[:, :width], axis=1, keepdims=True))
    questions = questions_ref[...].astype(jnp.bfloat16)
    inv_sqrt = width ** (-0.5)
    is_first = seq_index() == 0
    fresh_score = jnp.where(is_first, jnp.concatenate(fresh_scores, axis=0) * inv_sqrt, lowest_score)
    first_slot = seq_index() * (tokens // chunk)
    table = table_ref[...]
    row = lax.broadcasted_iota(jnp.int32, table.shape, 0)
    lengths = jnp.zeros(table.shape, jnp.int32)
    for b in range(requests):
        lengths = jnp.where(row == b, lengths_ref[b], lengths)
    left = jnp.clip(
        lengths - lax.broadcasted_iota(jnp.int32, table.shape, 1) * block_len, 0, block_len
    )
    place = lax.broadcasted_iota(jnp.int32, (requests, chunk), 1)
    limit = jnp.where(place % 2 == 0, place // 2, block_len)
    top = fresh_score
    hidden_from = []
    for k in range(tokens // chunk):
        filled = jnp.sum(jnp.where(table == first_slot + k, left, 0), axis=1, keepdims=True)
        visible = jnp.concatenate([(limit < filled).astype(F32)] * group_size, axis=0) > 0.5
        hidden_from.append(visible)
        scores = against_rows(questions, kv_ref[k * chunk : (k + 1) * chunk, :]) * inv_sqrt
        scores = jnp.where(visible, scores, lowest_score)
        scores_ref[:, k * chunk : (k + 1) * chunk] = scores
        top = jnp.maximum(top, jnp.max(scores, axis=1, keepdims=True))
    high, low = two_parts(top)
    top = high + low.astype(WIRE).astype(F32)
    weight = jnp.where(is_first, jnp.exp(fresh_score - top), 0.0)
    total = weight
    values = jnp.concatenate([fresh[:, width:]] * group_size, axis=0)
    mixed = weight * values
    for k in range(tokens // chunk):
        weight = jnp.where(
            hidden_from[k], jnp.exp(scores_ref[:, k * chunk : (k + 1) * chunk] - top), 0.0
        )
        total = total + jnp.sum(weight, axis=1, keepdims=True)
        moved = pltpu.roll(weight, 1, 1).astype(jnp.bfloat16)
        mixed = mixed + jnp.dot(moved, kv_ref[k * chunk : (k + 1) * chunk, :], preferred_element_type=F32)
    store_part(part_ref, flip(top), flip(total), mixed)


def merge_body(arrived_ref, part_ref):
    top, total, mixed = merged(arrived_ref)
    store_part(part_ref, top, total, mixed)


def attention_out_body(arrived_ref, weight_ref, sums_ref):
    _, total, mixed = merged(arrived_ref)
    attended = (mixed / flip(total)).astype(jnp.bfloat16)
    requests = sums_ref.shape[1]
    width = attended.shape[1]
    result = jnp.zeros(sums_ref.shape[1:], F32)
    for g in range(attended.shape[0] // requests):
        result = result + jnp.dot(
            attended[g * requests : (g + 1) * requests],
            weight_ref[g * width : (g + 1) * width, :],
            preferred_element_type=F32,
        )
    store_copies(sums_ref, result.astype(WIRE))


def last_body(arrived_ref, stream_ref, fresh_ref, out_ref, pair_ref):
    head = pair_ref.shape[3]
    for b in range(pair_ref.shape[0]):
        pair_ref[b, 0] = jnp.concatenate(
            [fresh_ref[b : b + 1, :head], fresh_ref[b : b + 1, head:]], axis=0
        ).astype(jnp.bfloat16)
    total = jnp.zeros((8, 128), F32)
    for k in range(arrived_ref.shape[0] // 8):
        total = total + arrived_ref[k * 8 : (k + 1) * 8, :].astype(F32)
    total = total + pltpu.roll(total, 4, 0)
    total = total + pltpu.roll(total, 2, 0)
    row = lax.broadcasted_iota(jnp.int32, (8, 128), 0)
    added = total
    for k in range(1, 4):
        added = jnp.where(row // 2 == k, pltpu.roll(total, 128 - 32 * k, 1), added)
    place = lax.axis_index("y") * lax.axis_size("core") + lax.axis_index("core")
    width = out_ref.shape[1]
    stream = stream_ref[...].astype(F32)
    own = stream[:, :width]
    for k in range(1, stream.shape[1] // width):
        own = jnp.where(place == k, stream[:, k * width : (k + 1) * width], own)
    out_ref[...] = (own + added[:, :width]).astype(jnp.bfloat16)


def shards(
    hidden,
    norm_gain,
    in_weight,
    conv_weight,
    conv_bias,
    conv_state,
    xproj_weight,
    dt_weight,
    dt_bias,
    a_log,
    skip_gain,
    ssm_state,
    out_weight,
    asker_lookup_matrix,
    o_weight,
    kv_cache,
    lengths,
    page_table,
):
    requests, model_dim = hidden.shape
    block_cols = model_dim // lax.axis_size(SEQ)
    share_cols = block_cols // lax.axis_size(CHAN)
    pages_dev, block_len, pair, _, width = kv_cache.shape
    entries = asker_lookup_matrix.shape[2]
    rows = requests * (entries // width - 2)
    in_rows = far(in_weight.transpose(0, 2, 3, 1))
    dt_rows = dt_weight.transpose(0, 2, 1)
    past = conv_state.transpose(0, 2, 1, 3)
    kv_rows = kv_cache.reshape(pages_dev * block_len * pair, width)
    conv_args = (conv_weight, conv_bias, past, xproj_weight)
    state_args = (dt_bias, a_log, skip_gain, out_weight)
    matrix = asker_lookup_matrix.reshape(block_cols, entries)

    def sums_of_proj(terms):
        own = jnp.sum(exchange(terms, PLANE).astype(F32), axis=0).astype(WIRE)
        return exchange(copied(own, LINE), LINE)

    terms, signal, gate, new_conv, own_block, own_gain = mamba_in(
        far(hidden), 0, far(norm_gain), in_rows, *[far(x) for x in conv_args], None
    )
    arrived, new_ssm = mamba_out(
        sums_of_proj(terms), signal, gate, 0, dt_rows, ssm_state, *state_args, None
    )
    stream_one, terms = local_call(
        questions_body,
        [
            (arrived, None),
            (own_block, None),
            (own_gain, None),
            (matrix, None),
        ],
        [
            ((requests, block_cols), jnp.bfloat16, None),
            ((lax.axis_size("x"), requests, entries + 128), WIRE, None),
        ],
    )
    own = jnp.sum(exchange(terms, "x").astype(F32), axis=0).astype(WIRE)
    part, fresh = local_call(
        functools.partial(attention_body, block_len=block_len, dim=model_dim),
        [
            (exchange(copied(own, "z"), "z"), None),
            (kv_rows, None),
            (lengths, "scalar"),
            (page_table, None),
        ],
        [
            ((lax.axis_size("x"), rows + 8, width), WIRE, None),
            ((requests, 2 * width), F32, None),
        ],
        [pltpu.VMEM((rows, width), F32), pltpu.VMEM((rows, kv_rows.shape[0]), F32)],
    )
    (part,) = local_call(
        merge_body,
        [(exchange(part, "x"), None)],
        [((lax.axis_size("z"), rows + 8, width), WIRE, None)],
    )
    (sums,) = local_call(
        attention_out_body,
        [(exchange(part, "z"), None), (o_weight[0], None)],
        [((lax.axis_size(CHAN), requests, block_cols), WIRE, None)],
    )
    added = jnp.sum(exchange(sums, CHAN_SUM).astype(F32), axis=0)
    stream_two = (stream_one.astype(F32) + added).astype(jnp.bfloat16)
    terms, signal, gate, new_conv = mamba_in(
        exchange(copied(stream_two, SEQ), SEQ), 1, norm_gain, in_rows, *conv_args, new_conv
    )
    arrived, new_ssm = mamba_out(
        sums_of_proj(terms), signal, gate, 1, dt_rows, ssm_state, *state_args, new_ssm
    )
    hidden_out, newest_pair = local_call(
        last_body,
        [(arrived, None), (stream_two, None), (fresh, None)],
        [
            ((requests, share_cols), jnp.bfloat16, None),
            ((requests, 1, 2, width), jnp.bfloat16, None),
        ],
    )
    return hidden_out, new_ssm, new_conv.transpose(0, 2, 1, 3), newest_pair


def solution(mesh):
    split = Mesh(mesh.devices.reshape(8, 4, 4, 2), ALL)
    placed = (
        P(),
        P(),
        P(None, None, None, ALL),
        P(None, None, ALL),
        P(None, ALL),
        P(None, None, None, ALL),
        P(None, ALL, None),
        P(None, None, ALL),
        P(None, ALL),
        P(None, None, ALL),
        P(None, ALL),
        P(None, None, None, ALL),
        P(None, ALL, None),
        P(SEQ, CHAN, None),
        P(CHAN, None, SEQ),
        P(SEQ, None, None, CHAN, None),
        P(),
        P(),
    )
    return jax.shard_map(
        shards,
        mesh=split,
        in_specs=placed,
        out_specs=(
            P(None, ALL),
            P(None, None, None, ALL),
            P(None, None, None, ALL),
            P(None, CHAN, None, None),
        ),
        check_vma=False,
    )
```

```python
import functools

import jax
import jax.numpy as jnp
from jax import lax
from jax.experimental import pallas as pl
from jax.experimental.pallas import tpu as pltpu
from jax.sharding import Mesh
from jax.sharding import PartitionSpec as P

ALL = ("z", "x", "y", "core")
SEQ = ("z", "x")
SEQ_SUM = ("x", "z")
CHAN = ("y", "core")
CHAN_SUM = ("core", "y")
PLANE = ("x", "y")
LINE = ("core", "z")
CORE_FIRST = ("core", "z", "x", "y")
WIRE = jnp.bfloat16
F32 = jnp.float32

norm_eps = 1e-06
lowest_score = -1e30


def exchange(copies, axes):
    return lax.all_to_all(copies, axes, split_axis=0, concat_axis=0, tiled=True)


def copied(x, axes):
    return jnp.broadcast_to(x, (lax.axis_size(axes), *x.shape))


def whole(shape):
    return pl.BlockSpec(shape, lambda _: (0,) * len(shape))


def layer_of(shape, layer):
    return pl.BlockSpec((1, *shape[1:]), lambda _: (layer,) + (0,) * (len(shape) - 1))


def far(x):
    return pltpu.with_memory_space_constraint(x, pltpu.HBM)


def local_call(body, inputs, outputs, scratch=(), aliases={}):
    def spec(shape, layer):
        if layer in ("far", "scalar"):
            return pl.BlockSpec(memory_space=pltpu.HBM if layer == "far" else pltpu.SMEM)
        return whole(shape) if layer is None else layer_of(shape, layer)

    return pl.pallas_call(
        body,
        grid=(1,),
        in_specs=[spec(x.shape, layer) for x, layer in inputs],
        out_specs=[spec(shape, layer) for shape, _, layer in outputs],
        out_shape=[jax.ShapeDtypeStruct(shape, dtype) for shape, dtype, _ in outputs],
        scratch_shapes=list(scratch),
        input_output_aliases=aliases,
        compiler_params=pltpu.CompilerParams(vmem_limit_bytes=12 * 1024 * 1024),
    )(*[x for x, _ in inputs])


def silu(x):
    return x * lax.logistic(x)


def added_up(ref):
    total = ref[0].astype(F32)
    for k in range(1, ref.shape[0]):
        total = total + ref[k].astype(F32)
    return total


def store_copies(ref, x):
    for k in range(ref.shape[0]):
        ref[k] = x


def against_rows(a, b):
    return lax.dot_general(a, b, (((1,), (1,)), ((), ())), preferred_element_type=F32)


def mamba_in_body(layer, *refs):
    stream_ref, gain_ref, in_ref, taps_ref, bias_ref, past_ref, xproj_ref = refs[:7]
    normed_ref, held_ref, done = refs[-3:]
    terms_ref, signal_ref, gate_ref, conv_ref = refs[7:11] if layer == 0 else refs[8:12]
    dim = normed_ref.shape[1]
    pieces = done.shape[0]
    piece = dim // pieces
    copies = [
        pltpu.make_async_copy(
            in_ref.at[layer, :, :, pl.ds(k * piece, piece)],
            held_ref.at[:, :, pl.ds(k * piece, piece)],
            done.at[k],
        )
        for k in range(pieces)
    ]
    for copy in copies:
        copy.start()
    if layer == 0:
        own_ref, own_gain_ref = refs[11:13]
        width = own_ref.shape[1]
        first = pl.multiple_of(seq_index() * width, width)
        own_ref[...] = stream_ref[:, pl.ds(first, width)]
        own_gain_ref[...] = gain_ref[1:2, pl.ds(first, width)]
    gain_row = (0, None, 2)[2 * layer]
    if len(stream_ref.shape) == 2:
        x = stream_ref[...].astype(F32)
        inv_rms = lax.rsqrt(jnp.sum(x * x, axis=1, keepdims=True) / dim + norm_eps)
        normed_ref[...] = (x * inv_rms * gain_ref[gain_row : gain_row + 1, :]).astype(jnp.bfloat16)
    else:
        blocks, _, width = stream_ref.shape
        squares = jnp.zeros(stream_ref.shape[1:], F32)
        for k in range(blocks):
            x = stream_ref[k].astype(F32)
            squares = squares + x * x
        inv_rms = lax.rsqrt(jnp.sum(squares, axis=1, keepdims=True) / dim + norm_eps)
        for k in range(blocks):
            cols = slice(k * width, (k + 1) * width)
            normed_ref[:, cols] = (
                stream_ref[k].astype(F32) * inv_rms * gain_ref[gain_row : gain_row + 1, cols]
            ).astype(jnp.bfloat16)
    inputs = jnp.zeros(signal_ref.shape, F32)
    gates = jnp.zeros(signal_ref.shape, F32)
    for k, copy in enumerate(copies):
        copy.wait()
        cols = slice(k * piece, (k + 1) * piece)
        normed = normed_ref[:, cols]
        inputs = inputs + against_rows(normed, held_ref[0, :, cols])
        gates = gates + against_rows(normed, held_ref[1, :, cols])
    inputs = inputs.astype(jnp.bfloat16)
    gates = gates.astype(jnp.bfloat16)
    taps = taps_ref[0]
    conv_sum = inputs.astype(F32) * taps[3:4]
    for k in range(3):
        conv_sum = conv_sum + past_ref[0, k].astype(F32) * taps[k : k + 1]
    signal = silu(conv_sum + bias_ref[layer : layer + 1, :]).astype(jnp.bfloat16)
    terms = jnp.dot(signal, xproj_ref[0], preferred_element_type=F32)
    store_copies(terms_ref, terms.astype(WIRE))
    signal_ref[...] = signal.astype(F32)
    gate_ref[...] = silu(gates.astype(F32))
    conv_ref[0, 0] = past_ref[0, 1]
    conv_ref[0, 1] = past_ref[0, 2]
    conv_ref[0, 2] = inputs


def mamba_in(
    stream, layer, norm_gain, in_rows, conv_weight, conv_bias, past, xproj_weight, conv_so_far
):
    requests = past.shape[2]
    channels = past.shape[3]
    inputs = [
        (stream, None),
        (norm_gain, None),
        (in_rows, "far"),
        (conv_weight, layer),
        (conv_bias, None),
        (past, layer),
        (xproj_weight, layer),
    ]
    aliases = {}
    if conv_so_far is not None:
        aliases = {len(inputs): 3}
        inputs.append((conv_so_far, "far"))
    extra = []
    if layer == 0:
        width = stream.shape[1] // lax.axis_size(SEQ)
        extra = [((requests, width), jnp.bfloat16, None), ((1, width), F32, None)]
    return local_call(
        functools.partial(mamba_in_body, layer),
        inputs,
        [
            ((lax.axis_size(PLANE), requests, xproj_weight.shape[2]), WIRE, None),
            ((requests, channels), F32, None),
            ((requests, channels), F32, None),
            (past.shape, jnp.bfloat16, layer),
            *extra,
        ],
        [
            pltpu.VMEM((requests, in_rows.shape[3]), jnp.bfloat16),
            pltpu.VMEM(in_rows.shape[1:], jnp.bfloat16),
            pltpu.SemaphoreType.DMA((4,)),
        ],
        aliases,
    )


def store_shares(shares_ref, block, x):
    row = lax.broadcasted_iota(jnp.int32, (8, 128), 0)
    group = lax.broadcasted_iota(jnp.int32, (8, 128), 1) // 32
    own = row // 2 == group
    packed = []
    for half in range(2):
        tile = x[:, half * 128 : (half + 1) * 128]
        turned = [tile] + [pltpu.roll(tile, 32 * k, 1) for k in range(1, 4)]
        for q in range(4):
            z = turned[-q % 4]
            for g in range(1, 4):
                z = jnp.where(group == g, turned[(g - q) % 4], z)
            z = jnp.where(own, z, 0.0)
            z = z + pltpu.roll(z, 4, 0)
            packed.append(z + pltpu.roll(z, 2, 0))
    for core in range(2):
        lines = packed[core]
        for k in range(1, 4):
            lines = jnp.where(row // 2 == k, packed[2 * k + core], lines)
        shares_ref[core, block * 8 : block * 8 + 8, :] = lines.astype(WIRE)


def mamba_out_body(layer, order, *refs):
    arrived_ref, signal_ref, gate_ref, dt_ref, bias_ref, decay_ref, skip_ref, state_ref, out_ref = (
        refs[:9]
    )
    blocks_ref, fresh_ref = refs[9:11] if layer == 0 else refs[10:12]
    if layer == 0:
        held_ref, done = refs[11:]
    else:
        held_ref = out_ref.at[0]
    pieces = 2 if layer == 0 else 0
    piece = out_ref.shape[2] // max(pieces, 1)
    copies = [
        pltpu.make_async_copy(
            out_ref.at[layer, :, pl.ds(k * piece, piece)],
            held_ref.at[:, pl.ds(k * piece, piece)],
            done.at[k],
        )
        for k in range(pieces)
    ]
    for copy in copies:
        copy.start()
    mapped = added_up(arrived_ref)
    low_rank = dt_ref.shape[2]
    states = decay_ref.shape[1]
    low = mapped[:, :low_rank].astype(jnp.bfloat16)
    raw = against_rows(low, dt_ref[0]) + bias_ref[layer : layer + 1, :]
    step = jnp.maximum(raw, 0.0) + jnp.log1p(jnp.exp(-jnp.abs(raw)))
    signal = signal_ref[...]
    pushed = step * signal
    rates = jnp.exp(decay_ref[0])
    rest = mapped[:, low_rank:]
    eye = lax.broadcasted_iota(jnp.int32, (states, states), 0) == lax.broadcasted_iota(
        jnp.int32, (states, states), 1
    )

    def column(row):
        return jnp.sum(jnp.where(eye, row, 0.0), axis=1, keepdims=True)

    readouts = []
    for b in range(mapped.shape[0]):
        b_in = column(rest[b : b + 1, :states])
        c_out = column(rest[b : b + 1, states : 2 * states])
        fresh = (
            jnp.exp(-step[b : b + 1] * rates) * state_ref[0, b] + pushed[b : b + 1] * b_in
        )
        fresh_ref[0, b] = fresh
        readouts.append(jnp.sum(fresh * c_out, axis=0, keepdims=True))
    readout = jnp.concatenate(readouts, axis=0) + skip_ref[layer : layer + 1, :] * signal
    gated = (readout * gate_ref[...]).astype(jnp.bfloat16)
    width = out_ref.shape[2] // len(order)
    for block in range(len(order)):
        if layer == 0 and block * width % piece == 0:
            copies[block * width // piece].wait()
        result = jnp.dot(
            gated,
            held_ref[:, block * width : (block + 1) * width],
            preferred_element_type=F32,
        )
        if layer == 0:
            blocks_ref[order.index(block)] = result.astype(WIRE)
        else:
            store_shares(blocks_ref, block, result)


def mamba_out(
    arrived, signal, gate, layer, dt_rows, ssm_state, dt_bias, a_log, skip_gain, out_weight, so_far
):
    wide, deep = (lax.axis_size(axis) for axis in SEQ_SUM)
    order = [k * wide + j for j in range(wide) for k in range(deep)]
    inputs = [
        (arrived, None),
        (signal, None),
        (gate, None),
        (dt_rows, min(layer, dt_rows.shape[0] - 1)),
        (dt_bias, None),
        (a_log, layer),
        (skip_gain, None),
        (ssm_state, min(layer, ssm_state.shape[0] - 1)),
        (far(out_weight), "far") if layer == 0 else (out_weight, layer),
    ]
    aliases = {}
    if so_far is not None:
        aliases = {len(inputs): 1}
        inputs.append((so_far, "far"))
    blocks, fresh = local_call(
        functools.partial(mamba_out_body, layer, order),
        inputs,
        [
            (
                (wide * deep, signal.shape[0], out_weight.shape[2] // (wide * deep))
                if layer == 0
                else (2, lax.axis_size(ALL), 128),
                WIRE,
                None,
            ),
            ((a_log.shape[0], *ssm_state.shape[1:]), F32, layer),
        ],
        [pltpu.VMEM(out_weight.shape[1:], jnp.bfloat16), pltpu.SemaphoreType.DMA((2,))]
        if layer == 0
        else [],
        aliases,
    )
    if layer:
        shares = exchange(blocks.reshape(-1, 2, 128), CORE_FIRST)
        return shares.reshape(-1, 128), fresh
    arrived = exchange(blocks, SEQ_SUM)
    own = jnp.sum(arrived.astype(F32), axis=0).astype(WIRE)
    return exchange(copied(own, CHAN_SUM), CHAN_SUM), fresh


def two_parts(x):
    high = x.astype(WIRE).astype(F32)
    return high, x - high


def questions_body(arrived_ref, hidden_ref, gain_ref, matrix_ref, stream_ref, terms_ref):
    stream = (hidden_ref[...].astype(F32) + added_up(arrived_ref)).astype(jnp.bfloat16)
    stream_ref[...] = stream
    wide = stream.astype(F32)
    high, low = two_parts(jnp.sum(wide * wide, axis=1, keepdims=True))
    scaled = (wide * gain_ref[...]).astype(jnp.bfloat16)
    terms = jnp.dot(scaled, matrix_ref[...], preferred_element_type=F32)
    lane = lax.broadcasted_iota(jnp.int32, (stream.shape[0], 128), 1)
    notes = jnp.where(lane == 0, high, jnp.where(lane == 1, low, 0.0))
    entries = terms.shape[1]
    for k in range(terms_ref.shape[0]):
        terms_ref[k, :, :entries] = terms.astype(WIRE)
        terms_ref[k, :, entries:] = notes.astype(WIRE)


def seq_index():
    return lax.axis_index("z") * lax.axis_size("x") + lax.axis_index("x")


def flip(x):
    n = max(x.shape)
    eye = lax.broadcasted_iota(jnp.int32, (n, n), 0) == lax.broadcasted_iota(jnp.int32, (n, n), 1)
    return jnp.sum(jnp.where(eye, x, 0.0), axis=x.shape.index(n), keepdims=True)


def store_part(out_ref, top, total, mixed):
    rows, width = mixed.shape
    high, low = two_parts(top)
    pad = jnp.zeros((1, width - rows), F32)
    notes = [jnp.concatenate([v, pad], axis=1) for v in (high, low, total)]
    notes = jnp.concatenate([*notes, jnp.zeros((out_ref.shape[1] - rows - 3, width), F32)], axis=0)
    for k in range(out_ref.shape[0]):
        out_ref[k, :rows, :] = mixed.astype(WIRE)
        out_ref[k, rows:, :] = notes.astype(WIRE)


def merged(arrived_ref):
    parts, stored, _ = arrived_ref.shape
    rows = stored - 8
    notes = [arrived_ref[k, rows:, :].astype(F32) for k in range(parts)]
    tops = [v[0:1, :rows] + v[1:2, :rows] for v in notes]
    top = tops[0]
    for v in tops[1:]:
        top = jnp.maximum(top, v)
    total = jnp.zeros_like(top)
    mixed = jnp.zeros((rows, arrived_ref.shape[2]), F32)
    for k in range(parts):
        scale = jnp.exp(tops[k] - top)
        total = total + scale * notes[k][2:3, :rows]
        mixed = mixed + flip(scale) * arrived_ref[k, :rows, :].astype(F32)
    return top, total, mixed


def attention_body(
    arrived_ref, kv_ref, lengths_ref, table_ref, part_ref, pair_ref, questions_ref, scores_ref, *, block_len, dim
):
    summed = added_up(arrived_ref)
    requests = summed.shape[0]
    width = kv_ref.shape[1]
    entries = summed.shape[1] - 128
    group_size = entries // width - 2
    rows = requests * group_size
    tokens = kv_ref.shape[0]
    chunk = 2 * block_len
    inv_rms = lax.rsqrt((summed[:, entries : entries + 1] + summed[:, entries + 1 : entries + 2]) / dim + norm_eps)
    qkv = (summed[:, :entries] * inv_rms).astype(jnp.bfloat16)
    fresh = qkv[:, group_size * width :]
    fresh = fresh.astype(F32)
    pair_ref[...] = fresh
    fresh_scores = []
    for g in range(group_size):
        one = qkv[:, g * width : (g + 1) * width]
        questions_ref[g * requests : (g + 1) * requests, :] = one.astype(F32)
        fresh_scores.append(jnp.sum(one.astype(F32) * fresh[:, :width], axis=1, keepdims=True))
    questions = questions_ref[...].astype(jnp.bfloat16)
    inv_sqrt = width ** (-0.5)
    is_first = seq_index() == 0
    fresh_score = jnp.where(is_first, jnp.concatenate(fresh_scores, axis=0) * inv_sqrt, lowest_score)
    first_slot = seq_index() * (tokens // chunk)
    table = table_ref[...]
    row = lax.broadcasted_iota(jnp.int32, table.shape, 0)
    lengths = jnp.zeros(table.shape, jnp.int32)
    for b in range(requests):
        lengths = jnp.where(row == b, lengths_ref[b], lengths)
    left = jnp.clip(
        lengths - lax.broadcasted_iota(jnp.int32, table.shape, 1) * block_len, 0, block_len
    )
    place = lax.broadcasted_iota(jnp.int32, (requests, chunk), 1)
    limit = jnp.where(place % 2 == 0, place // 2, block_len)
    top = fresh_score
    hidden_from = []
    for k in range(tokens // chunk):
        filled = jnp.sum(jnp.where(table == first_slot + k, left, 0), axis=1, keepdims=True)
        visible = jnp.concatenate([(limit < filled).astype(F32)] * group_size, axis=0) > 0.5
        hidden_from.append(visible)
        scores = against_rows(questions, kv_ref[k * chunk : (k + 1) * chunk, :]) * inv_sqrt
        scores = jnp.where(visible, scores, lowest_score)
        scores_ref[:, k * chunk : (k + 1) * chunk] = scores
        top = jnp.maximum(top, jnp.max(scores, axis=1, keepdims=True))
    high, low = two_parts(top)
    top = high + low.astype(WIRE).astype(F32)
    weight = jnp.where(is_first, jnp.exp(fresh_score - top), 0.0)
    total = weight
    values = jnp.concatenate([fresh[:, width:]] * group_size, axis=0)
    mixed = weight * values
    for k in range(tokens // chunk):
        weight = jnp.where(
            hidden_from[k], jnp.exp(scores_ref[:, k * chunk : (k + 1) * chunk] - top), 0.0
        )
        total = total + jnp.sum(weight, axis=1, keepdims=True)
        moved = pltpu.roll(weight, 1, 1).astype(jnp.bfloat16)
        mixed = mixed + jnp.dot(moved, kv_ref[k * chunk : (k + 1) * chunk, :], preferred_element_type=F32)
    store_part(part_ref, flip(top), flip(total), mixed)


def merge_body(arrived_ref, part_ref):
    top, total, mixed = merged(arrived_ref)
    store_part(part_ref, top, total, mixed)


def attention_out_body(arrived_ref, far_ref, sums_ref, weight_ref, done):
    copy = pltpu.make_async_copy(far_ref, weight_ref, done.at[0])
    copy.start()
    _, total, mixed = merged(arrived_ref)
    attended = (mixed / flip(total)).astype(jnp.bfloat16)
    requests = sums_ref.shape[1]
    width = attended.shape[1]
    result = jnp.zeros(sums_ref.shape[1:], F32)
    copy.wait()
    for g in range(attended.shape[0] // requests):
        result = result + jnp.dot(
            attended[g * requests : (g + 1) * requests],
            weight_ref[g * width : (g + 1) * width, :],
            preferred_element_type=F32,
        )
    store_copies(sums_ref, result.astype(WIRE))


def last_body(arrived_ref, stream_ref, fresh_ref, out_ref, pair_ref):
    head = pair_ref.shape[3]
    for b in range(pair_ref.shape[0]):
        pair_ref[b, 0] = jnp.concatenate(
            [fresh_ref[b : b + 1, :head], fresh_ref[b : b + 1, head:]], axis=0
        ).astype(jnp.bfloat16)
    total = jnp.zeros((8, 128), F32)
    for k in range(arrived_ref.shape[0] // 8):
        total = total + arrived_ref[k * 8 : (k + 1) * 8, :].astype(F32)
    total = total + pltpu.roll(total, 4, 0)
    total = total + pltpu.roll(total, 2, 0)
    row = lax.broadcasted_iota(jnp.int32, (8, 128), 0)
    added = total
    for k in range(1, 4):
        added = jnp.where(row // 2 == k, pltpu.roll(total, 128 - 32 * k, 1), added)
    place = lax.axis_index("y") * lax.axis_size("core") + lax.axis_index("core")
    width = out_ref.shape[1]
    stream = stream_ref[...].astype(F32)
    own = stream[:, :width]
    for k in range(1, stream.shape[1] // width):
        own = jnp.where(place == k, stream[:, k * width : (k + 1) * width], own)
    out_ref[...] = (own + added[:, :width]).astype(jnp.bfloat16)


def shards(
    hidden,
    norm_gain,
    in_weight,
    conv_weight,
    conv_bias,
    conv_state,
    xproj_weight,
    dt_weight,
    dt_bias,
    a_log,
    skip_gain,
    ssm_state,
    out_weight,
    asker_lookup_matrix,
    o_weight,
    kv_cache,
    lengths,
    page_table,
):
    requests, model_dim = hidden.shape
    block_cols = model_dim // lax.axis_size(SEQ)
    share_cols = block_cols // lax.axis_size(CHAN)
    pages_dev, block_len, pair, _, width = kv_cache.shape
    entries = asker_lookup_matrix.shape[2]
    rows = requests * (entries // width - 2)
    in_rows = far(in_weight.transpose(0, 2, 3, 1))
    dt_rows = dt_weight.transpose(0, 2, 1)
    past = conv_state.transpose(0, 2, 1, 3)
    kv_rows = kv_cache.reshape(pages_dev * block_len * pair, width)
    conv_args = (conv_weight, conv_bias, past, xproj_weight)
    state_args = (dt_bias, a_log, skip_gain, out_weight)
    matrix = asker_lookup_matrix.reshape(block_cols, entries)

    def sums_of_proj(terms):
        own = jnp.sum(exchange(terms, PLANE).astype(F32), axis=0).astype(WIRE)
        return exchange(copied(own, LINE), LINE)

    terms, signal, gate, new_conv, own_block, own_gain = mamba_in(
        far(hidden), 0, far(norm_gain), in_rows, *[far(x) for x in conv_args], None
    )
    arrived, new_ssm = mamba_out(
        sums_of_proj(terms), signal, gate, 0, dt_rows, ssm_state, *state_args, None
    )
    stream_one, terms = local_call(
        questions_body,
        [
            (arrived, None),
            (own_block, None),
            (own_gain, None),
            (matrix, None),
        ],
        [
            ((requests, block_cols), jnp.bfloat16, None),
            ((lax.axis_size("x"), requests, entries + 128), WIRE, None),
        ],
    )
    own = jnp.sum(exchange(terms, "x").astype(F32), axis=0).astype(WIRE)
    part, fresh = local_call(
        functools.partial(attention_body, block_len=block_len, dim=model_dim),
        [
            (exchange(copied(own, "z"), "z"), None),
            (kv_rows, None),
            (lengths, "scalar"),
            (page_table, None),
        ],
        [
            ((lax.axis_size("x"), rows + 8, width), WIRE, None),
            ((requests, 2 * width), F32, None),
        ],
        [pltpu.VMEM((rows, width), F32), pltpu.VMEM((rows, kv_rows.shape[0]), F32)],
    )
    (part,) = local_call(
        merge_body,
        [(exchange(part, "x"), None)],
        [((lax.axis_size("z"), rows + 8, width), WIRE, None)],
    )
    (sums,) = local_call(
        attention_out_body,
        [(exchange(part, "z"), None), (far(o_weight[0]), "far")],
        [((lax.axis_size(CHAN), requests, block_cols), WIRE, None)],
        [pltpu.VMEM(o_weight.shape[1:], jnp.bfloat16), pltpu.SemaphoreType.DMA((1,))],
    )
    added = jnp.sum(exchange(sums, CHAN_SUM).astype(F32), axis=0)
    stream_two = (stream_one.astype(F32) + added).astype(jnp.bfloat16)
    terms, signal, gate, new_conv = mamba_in(
        exchange(copied(stream_two, SEQ), SEQ), 1, norm_gain, in_rows, *conv_args, new_conv
    )
    arrived, new_ssm = mamba_out(
        sums_of_proj(terms), signal, gate, 1, dt_rows, ssm_state, *state_args, new_ssm
    )
    hidden_out, newest_pair = local_call(
        last_body,
        [(arrived, None), (stream_two, None), (fresh, None)],
        [
            ((requests, share_cols), jnp.bfloat16, None),
            ((requests, 1, 2, width), jnp.bfloat16, None),
        ],
    )
    return hidden_out, new_ssm, new_conv.transpose(0, 2, 1, 3), newest_pair


def solution(mesh):
    split = Mesh(mesh.devices.reshape(8, 4, 4, 2), ALL)
    placed = (
        P(),
        P(),
        P(None, None, None, ALL),
        P(None, None, ALL),
        P(None, ALL),
        P(None, None, None, ALL),
        P(None, ALL, None),
        P(None, None, ALL),
        P(None, ALL),
        P(None, None, ALL),
        P(None, ALL),
        P(None, None, None, ALL),
        P(None, ALL, None),
        P(SEQ, CHAN, None),
        P(CHAN, None, SEQ),
        P(SEQ, None, None, CHAN, None),
        P(),
        P(),
    )
    return jax.shard_map(
        shards,
        mesh=split,
        in_specs=placed,
        out_specs=(
            P(None, ALL),
            P(None, None, None, ALL),
            P(None, None, None, ALL),
            P(None, CHAN, None, None),
        ),
        check_vma=False,
    )
```
